32 devices in a mesh: blk: 16 (over z, y, x), grp: 2 (over core).
Axes of the slice: x: 2, y: 2, z: 4, core: 2. Of those that a mesh axis runs over, the one named last changes fastest.
Arguments:
- sky_maps: float32 [4, 128, 4096], P(None, ('blk', 'grp')), may hold values from -6 to 6
- legendre: bfloat16 [128, 512, 2048], P(('blk', 'grp')), may hold values from -0.5 to 0.5
- owner_table: int32 [512], replicated, may hold values from 0 to 511, each once
Outputs:
- harmonics: float32 [512, 4, 2, 2048], P(('blk', 'grp'))
- spectra: float32 [10, 2048], P(None, ('blk', 'grp'))
The draws below stay inside these ranges and needn't reach their ends.
Inputs may be any that keep to these rules, and one draw needn't show every extreme that they name: `owner_table`: a permutation of the orders 0 to 511.
All inputs are finite; a program needn't handle non-finite values.
Results may differ from the reference program's by a relative error of at most 0.0034.
Values may be sent and summed in bfloat16 or wider, within the bound.
A program may use at most 128 MiB of HBM per device.

```python
import math
import jax
import jax.numpy as jnp
import numpy as np
from jax import lax

MAPS = 4
M = 512
L = 2048
NPHI = 4096
CYCLES = 128


def levels(own_key, shape, shards, smallest, top_value):
    def one(dim, blocks):
        heights = jax.random.uniform(jax.random.fold_in(jax.random.fold_in(own_key, 6), dim), (blocks,), jnp.float32, smallest / len(shards), top_value / len(shards))
        return jnp.repeat(jnp.exp(heights), shape[dim] // blocks).reshape((-1,) + (1,) * (len(shape) - dim - 1))

    loudness = one(*shards[0])
    for cut in shards[1:]:
        loudness = loudness * one(*cut)
    return loudness


def scatter_about(own_key, dims, scale, limit, pieces=(), kind=jnp.bfloat16):
    array = scale * jax.random.normal(own_key, dims, jnp.float32)
    if pieces:
        array = array * levels(own_key, dims, pieces, -0.22, 0.18)
    return jnp.clip(array, -limit, limit).astype(kind)


def setup_inputs(seed: int = 0) -> dict:
    seeds = jax.random.split(jax.random.key(seed), 4)
    sky_maps = scatter_about(seeds[0], (MAPS, CYCLES, NPHI), 1.0, 6.0, ((1, 32),), jnp.float32)
    legendre = scatter_about(seeds[1], (CYCLES, M, L), CYCLES ** -0.5, 0.5, ((0, 32),))
    owner_table = jax.random.permutation(seeds[2], M).astype(jnp.int32)
    return dict(sky_maps=sky_maps, legendre=legendre, owner_table=owner_table)


def reference(sky_maps, legendre, owner_table):
    coeffs = jnp.fft.rfft(sky_maps, axis=-1)[..., :M] / math.sqrt(NPHI)
    fourier = jnp.stack([jnp.real(coeffs), jnp.imag(coeffs)], axis=2)
    fourier = jnp.transpose(fourier, (1, 0, 2, 3)).reshape(CYCLES, 2 * MAPS, M).astype(jnp.bfloat16)
    ell_index = jnp.arange(L, dtype=jnp.int32)

    def per_block(orders):
        table = jnp.take(legendre, orders, axis=1).astype(jnp.float32)
        values = jnp.take(fourier, orders, axis=2).astype(jnp.float32)
        block = jnp.einsum('rcm,rml->mcl', values, table)
        keep = ell_index[None, None, :] >= orders[:, None, None]
        return jnp.where(keep, block, jnp.zeros_like(block))
    harmonics = lax.map(per_block, owner_table.reshape(M // 64, 64)).reshape(M, MAPS, 2, L)
    weight = jnp.where(owner_table == 0, jnp.float32(1.0), jnp.float32(2.0)).astype(jnp.float32)
    cross = jnp.einsum('m,miql,mjql->ijl', weight, harmonics, harmonics)
    first, second = np.triu_indices(MAPS)
    spectra = cross[first, second] / (2 * ell_index + 1).astype(jnp.float32)
    return (harmonics, spectra)
```

```python
import functools
import math

import jax
import jax.numpy as jnp
import numpy as np
from jax import lax
from jax.experimental import pallas as pl
from jax.experimental.pallas import tpu as pltpu
from jax.sharding import PartitionSpec as P

AXES = ("blk", "grp")
MIB = 1024 * 1024
MESH = pl.DeviceIdType.MESH
BF16 = jnp.bfloat16
F32 = jnp.float32
GROUP = 16
FIRST = (1, 2)
EARLY = 3
WIDTH = 256


def plan_of(bits):
    later = [[EARLY] + [b for b in range(1, bits) if b not in (first, EARLY)] for first in FIRST]
    return later


def flip(me, bits):
    out = me
    for b in bits:
        out = out + (1 - 2 * ((me // (1 << b)) % 2)) * (1 << b)
    return out


def split_bf16(values):
    high = values.astype(BF16)
    low = (values - high.astype(F32)).astype(BF16)
    return high, low


def dot(left, right):
    return jnp.dot(left, right, preferred_element_type=F32)


def dot_t(left, right):
    return lax.dot_general(left, right, (((1,), (1,)), ((), ())), preferred_element_type=F32)


def fourier_tables(pixels, order_count, width):
    coarse = pixels // width
    k1, m1 = np.meshgrid(np.arange(coarse), np.arange(coarse), indexing="ij")
    angle = 2.0 * math.pi * ((k1 * m1) % coarse) / coarse
    first = np.concatenate([np.cos(angle.T), -np.sin(angle.T)], axis=0)
    k2 = np.arange(width)[:, None]
    m = np.arange(order_count)[None, :]
    angle = 2.0 * math.pi * ((k2 * m) % pixels) / pixels
    cosine, sine = np.cos(angle) / math.sqrt(pixels), np.sin(angle) / math.sqrt(pixels)
    second = np.block([[cosine, -sine], [sine, cosine]]).astype(np.float32)
    high = second.astype(jnp.bfloat16)
    low = (second - high.astype(np.float32)).astype(jnp.bfloat16)
    return first.astype(np.float32), high, low


def kernel(
    cfg, owner_smem, owner_ref, sky_hbm, first_hbm, high_hbm, low_hbm, leg_hbm, harm_ref, spec_ref,
    leg_v, sky_v, first_v, high_v, low_v, hot_v, lhs_v, own0, send0, recv0, coef_own, coef_send, coef_recv,
    acc_v, halves, pow_v, pow_recv, pow_mine, pow_pair, load_sem, sky_sem, table_sem,
    sems0, coef_sems, half_sems, pow_sems, pair_sems,
):
    maps, cycles, orders, ells, devices, grp, width = cfg
    bits = devices.bit_length() - 1
    later = plan_of(bits)
    steps = bits - 2
    chunks = ells // width
    channels = 2 * maps
    own = orders // devices
    per_type = own // 2
    block = orders // 8
    rows0 = block * channels
    me = lax.axis_index("blk") * grp + lax.axis_index("grp")
    tile = 128
    tiles = ells // tile
    sharers = tile * devices // ells
    pairs = maps * (maps + 1) // 2

    def at(index):
        return (index // grp, index % grp)

    def bit(b):
        return (me // (1 << b)) % 2

    gather = [[None, flip(me, [0]), flip(me, [FIRST[ty]]), flip(me, [FIRST[ty], 0])] for ty in range(2)]
    near = sorted({(0,)} | {(f,) for f in FIRST} | {(0, f) for f in FIRST} | {(b,) for b in range(1, bits)})

    barrier = pltpu.get_barrier_semaphore()
    for masks in near:
        pl.semaphore_signal(barrier, inc=1, device_id=at(flip(me, masks)), device_id_type=MESH)

    def load(t):
        lanes = pl.ds(pl.multiple_of(t * width, width), width)
        return pltpu.make_async_copy(leg_hbm.at[:, :, lanes], leg_v.at[t], load_sem.at[t])

    def load_start(t, carry):
        load(t).start()
        return carry

    lax.fori_loop(0, chunks, load_start, 0)
    coarse = sky_v.shape[2]

    def sky_load(k):
        lanes = pl.ds(pl.multiple_of(k * tile, tile), tile)
        return pltpu.make_async_copy(sky_hbm.at[:, :, lanes], sky_v.at[:, :, k, :], sky_sem.at[k])

    def sky_start(k, carry):
        sky_load(k).start()
        return carry

    lax.fori_loop(0, coarse, sky_start, 0)
    tables = [
        pltpu.make_async_copy(src, dst, table_sem.at[i])
        for i, (src, dst) in enumerate(((first_hbm, first_v), (high_hbm, high_v), (low_hbm, low_v)))
    ]
    for table in tables:
        table.start()

    j = lax.broadcasted_iota(jnp.int32, (orders, tile), 0)
    part = j // (orders // 2)
    rest = j % block
    slot = part * per_type + rest % per_type

    def place(b, differs):
        mine = bit(b)
        return (mine + differs - 2 * mine * differs) * ((1 << b) * own)

    slot = slot + place(0, (j // block) % 2)
    for ty in range(2):
        terms = place(FIRST[ty], (j // (2 * block)) % 2)
        for s, b in enumerate(later[ty]):
            terms = terms + place(b, (rest // (block >> (s + 1))) % 2)
        slot = slot + jnp.where(part == ty, terms, 0)
    lane = lax.broadcasted_iota(jnp.int32, (orders, tile), 1)
    pick = jnp.concatenate(
        [jnp.where(slot == lane + c * tile, 1.0, 0.0).astype(BF16) for c in range(orders // tile)], axis=1
    )
    table = jnp.where(lax.broadcasted_iota(jnp.int32, (orders, orders), 0) == owner_ref[...], 1.0, 0.0).astype(BF16)
    hot_v[...] = dot_t(pick, table).astype(BF16)

    def gather_copy(ty, t, p):
        return pltpu.make_async_remote_copy(
            src_ref=send0.at[ty, t, p - 1],
            dst_ref=recv0.at[ty, t, p - 1],
            send_sem=sems0.at[0, ty, t, p - 1],
            recv_sem=sems0.at[1, ty, t, p - 1],
            device_id=at(gather[ty][p]),
            device_id_type=MESH,
        )

    def coef_copy(ty, p):
        return pltpu.make_async_remote_copy(
            src_ref=coef_send.at[ty, p - 1],
            dst_ref=coef_recv.at[ty, p - 1],
            send_sem=coef_sems.at[0, ty, p - 1],
            recv_sem=coef_sems.at[1, ty, p - 1],
            device_id=at(gather[ty][p]),
            device_id_type=MESH,
        )

    def half_copy(s, ty, t):
        return pltpu.make_async_remote_copy(
            src_ref=halves[2 * s].at[ty, t],
            dst_ref=halves[2 * s + 1].at[ty, t],
            send_sem=half_sems.at[0, s, ty, t],
            recv_sem=half_sems.at[1, s, ty, t],
            device_id=at(flip(me, [later[ty][s]])),
            device_id_type=MESH,
        )

    def permute(t):
        load(t).wait()
        for r in range(cycles):
            values = leg_v[t, r]
            for ty in range(2):
                picked = dot(hot_v[ty * 4 * block : (ty + 1) * 4 * block, :], values).astype(BF16)
                own0[ty, t, r] = picked[:block]
                for p in range(1, 4):
                    send0[ty, t, p - 1, r] = picked[p * block : (p + 1) * block]
        for p in (2, 3, 1):
            for ty in range(2):
                gather_copy(ty, t, p).start()

    pl.semaphore_wait(barrier, len(near))
    permute(0)

    def sky_wait(k, carry):
        sky_load(k).wait()
        return carry

    lax.fori_loop(0, coarse, sky_wait, 0)
    for table in tables:
        table.wait()
    count = maps * cycles
    columns = 2 * orders
    stages = []
    first = first_v[...]
    for b in range(count):
        stage = jnp.dot(
            first, sky_v[b // cycles, b % cycles], precision=lax.Precision.HIGHEST, preferred_element_type=F32
        )
        stages.append(jnp.concatenate([stage[:coarse], stage[coarse:]], axis=1))
    left_high, left_low = split_bf16(jnp.concatenate(stages, axis=0))
    spectral = []
    span = orders // 2
    for c in range(columns // span):
        picked = slice(c * span, (c + 1) * span)
        full = dot(left_high, high_v[:, picked]) + (dot(left_high, low_v[:, picked]) + dot(left_low, high_v[:, picked]))
        full = full.reshape(count, coarse, span)
        m1 = lax.broadcasted_iota(jnp.int32, (1, coarse, span), 1)
        col = lax.broadcasted_iota(jnp.int32, (1, coarse, span), 2)
        spectral.append(jnp.sum(jnp.where(col % coarse == m1, full, 0.0), axis=1))
    spectral = jnp.concatenate(
        [jnp.concatenate(spectral[:2], axis=1), jnp.concatenate(spectral[2:], axis=1)], axis=0
    ).astype(BF16)
    spectral = jnp.concatenate([spectral, jnp.zeros((tile - 2 * count, orders), BF16)], axis=0)
    coef = dot_t(hot_v[...], spectral).astype(BF16)
    for ty in range(2):
        base = ty * 4 * block
        coef_own[ty] = coef[base : base + block]
        for p in range(1, 4):
            coef_send[ty, p - 1] = coef[base + p * block : base + (p + 1) * block]
    for p in (2, 3, 1):
        for ty in range(2):
            coef_copy(ty, p).start()

    def permute_step(t, carry):
        permute(t)
        return carry

    lax.fori_loop(1, chunks, permute_step, 0)

    source = lax.broadcasted_iota(jnp.int32, (tile, cycles * tile), 0)
    target = lax.broadcasted_iota(jnp.int32, (tile, cycles * tile), 1)
    channel = 2 * ((source // cycles) % maps) + source // count
    same = (source % cycles == target // tile) & (channel == target % channels) & (source < 2 * count)
    expand = jnp.where(same, 1.0, 0.0).astype(BF16)
    depth = 4 * cycles * GROUP
    keep = lax.broadcasted_iota(jnp.int32, (depth, tile), 0) % GROUP == (
        lax.broadcasted_iota(jnp.int32, (depth, tile), 1) // channels
    )
    for ty in range(2):
        spread = []
        for p in range(4):
            if p:
                coef_copy(ty, p).wait_recv()
            values = coef_recv[ty, p - 1] if p else coef_own[ty]
            spread.append(dot(values, expand))
        for g in range(block // GROUP):
            pieces = [
                spread[p][g * GROUP : (g + 1) * GROUP, r * tile : (r + 1) * tile]
                for p in range(4)
                for r in range(cycles)
            ]
            stacked = jnp.where(keep, jnp.concatenate(pieces, axis=0), 0.0)
            lhs_v[ty, g] = stacked.T.astype(BF16)

    groups = block // GROUP
    high_rows = GROUP * channels

    def product(ty, t, g):
        span = slice(g * GROUP, (g + 1) * GROUP)
        parts = [own0[ty, t, :, span, :]] + [recv0[ty, t, p, :, span, :] for p in range(3)]
        right = jnp.concatenate([v.reshape(cycles * GROUP, width) for v in parts], axis=0)
        return dot(lhs_v[ty, g], right)

    def first_step(t):
        for ty in range(2):
            for p in range(1, 4):
                gather_copy(ty, t, p).wait_recv()
            for g in range(groups // 2, groups):
                at_row = (g - groups // 2) * high_rows
                halves[0][ty, t, at_row : at_row + high_rows, :] = product(ty, t, g).astype(BF16)
            half_copy(0, ty, t).start()
        for ty in range(2):
            for g in range(groups // 2):
                acc_v[ty, t, g * high_rows : (g + 1) * high_rows, :] = product(ty, t, g)

    def next_step(s, t):
        size = rows0 >> (s + 1)
        for ty in range(2):
            half_copy(s - 1, ty, t).wait_recv()
            got = halves[2 * s - 1]
            value = acc_v[ty, t, size : 2 * size, :] + got[ty, t, size:, :].astype(F32)
            halves[2 * s][ty, t] = value.astype(BF16)
            half_copy(s, ty, t).start()
            acc_v[ty, t, :size, :] = acc_v[ty, t, :size, :] + got[ty, t, :size, :].astype(F32)

    def pow_copy(u):
        return pltpu.make_async_remote_copy(
            src_ref=pow_v.at[u],
            dst_ref=pow_recv.at[me // sharers],
            send_sem=pow_sems.at[0, u],
            recv_sem=pow_sems.at[1, me // sharers],
            device_id=at(u * sharers + me % sharers),
            device_id_type=MESH,
        )

    def last_step(t):
        size = rows0 >> steps
        ell = t * width + lax.broadcasted_iota(jnp.int32, (channels, width), 1)
        total = [None] * (maps // 2 + 1)
        lanes = pl.ds(pl.multiple_of(t * width, width), width)
        for ty in range(2):
            half_copy(steps - 1, ty, t).wait_recv()
            value = acc_v[ty, t, :size, :] + halves[2 * steps - 1][ty, t].astype(F32)
            for i in range(per_type):
                order = owner_smem[me * own + ty * per_type + i]
                mode = jnp.where(ell >= order, value[i * channels : (i + 1) * channels], 0.0)
                row = (ty * per_type + i) * channels
                harm_ref[row : row + channels, lanes] = mode
                heavy = mode * jnp.where(order == 0, 1.0, 2.0)
                for k in range(maps // 2 + 1):
                    turned = mode if k == 0 else jnp.concatenate([mode[2 * k :], mode[: 2 * k]], axis=0)
                    term = heavy * turned
                    total[k] = term if total[k] is None else total[k] + term
        rows = []
        for i in range(maps):
            for jj in range(i, maps):
                k, a = (jj - i, i) if jj - i <= maps // 2 else (maps - (jj - i), jj)
                rows.append(total[k][2 * a : 2 * a + 1] + total[k][2 * a + 1 : 2 * a + 2])
        power = jnp.concatenate(rows + [jnp.zeros((pow_v.shape[1] - pairs, width), F32)], axis=0)
        for h in range(width // tile):
            u = t * (width // tile) + h
            pow_v[u] = power[:, h * tile : (h + 1) * tile]

            @pl.when(u != me // sharers)
            def _():
                pow_copy(u).start()

    def main(t, carry):
        @pl.when(t < chunks)
        def _():
            first_step(t)

        @pl.when(t > 0)
        def _():
            next_step(1, t - 1)

        return carry

    lax.fori_loop(0, chunks + 1, main, 0)
    for s in range(2, steps):

        def tail(t, carry):
            @pl.when(t < chunks)
            def _():
                next_step(s, t)

            if s == steps - 1:

                @pl.when(t > 0)
                def _():
                    last_step(t - 1)

            return carry

        lax.fori_loop(0, chunks + (s == steps - 1), tail, 0)

    mine = me // sharers
    total = pow_v[mine]
    for u in range(tiles):

        @pl.when(u != mine)
        def _():
            copy = pltpu.make_async_remote_copy(
                src_ref=pow_v.at[u],
                dst_ref=pow_recv.at[u],
                send_sem=pow_sems.at[0, u],
                recv_sem=pow_sems.at[1, u],
                device_id=at(u * sharers + me % sharers),
                device_id_type=MESH,
            )
            copy.wait_recv()

    for u in range(tiles):
        total = total + jnp.where(u != mine, pow_recv[u], 0.0)
    pow_mine[...] = total

    def pair_copy(e):
        return pltpu.make_async_remote_copy(
            src_ref=pow_mine,
            dst_ref=pow_pair.at[e - 1],
            send_sem=pair_sems.at[0, e - 1],
            recv_sem=pair_sems.at[1, e - 1],
            device_id=at(mine * sharers + (me + e) % sharers),
            device_id_type=MESH,
        )

    for e in range(1, sharers):
        pair_copy(e).start()
    for e in range(1, sharers):
        pair_copy(e).wait_recv()
        total = total + pow_pair[e - 1]
    ell = mine * tile + lax.broadcasted_iota(jnp.int32, total.shape, 1)
    total = total / (2 * ell + 1).astype(F32)
    share = tile // sharers
    turned = total
    for c in range(1, sharers):
        shifted = jnp.concatenate([total[:, c * share :], total[:, : c * share]], axis=1)
        turned = jnp.where(me % sharers == c, shifted, turned)
    spec_ref[...] = turned[:pairs, :share]

    def drain(t, carry):
        for ty in range(2):
            for p in range(1, 4):
                gather_copy(ty, t, p).wait_send()
            for s in range(steps):
                half_copy(s, ty, t).wait_send()
        return carry

    lax.fori_loop(0, chunks, drain, 0)
    for ty in range(2):
        for p in range(1, 4):
            coef_copy(ty, p).wait_send()
    for e in range(1, sharers):
        pair_copy(e).wait_send()
    for u in range(tiles):

        @pl.when(u != mine)
        def _():
            pow_copy(u).wait_send()


def per_device(sky_maps, legendre, owner_table):
    maps, cycles, pixels = sky_maps.shape
    _, orders, ells = legendre.shape
    devices = lax.axis_size(AXES)
    grp = lax.axis_size(AXES[1])
    bits = devices.bit_length() - 1
    steps = bits - 2
    width = WIDTH
    chunks = ells // width
    channels = 2 * maps
    own = orders // devices
    block = orders // 8
    tile = 128
    coarse = pixels // tile
    tiles = ells // tile
    sharers = tile * devices // ells
    pairs = maps * (maps + 1) // 2
    padded = -(-pairs // 8) * 8
    first, high, low = fourier_tables(pixels, orders, tile)
    rows0 = block * channels
    halves = []
    for s in range(steps):
        halves += [pltpu.VMEM((2, chunks, rows0 >> (s + 1), width), BF16)] * 2
    cfg = (maps, cycles, orders, ells, devices, grp, width)
    scratch = [
        pltpu.VMEM((chunks, cycles, orders, width), BF16),
        pltpu.VMEM((maps, cycles, coarse, tile), F32),
        pltpu.VMEM(first.shape, F32),
        pltpu.VMEM(high.shape, BF16),
        pltpu.VMEM(low.shape, BF16),
        pltpu.VMEM((orders, orders), BF16),
        pltpu.VMEM((2, block // GROUP, GROUP * channels, 4 * cycles * GROUP), BF16),
        pltpu.VMEM((2, chunks, cycles, block, width), BF16),
        pltpu.VMEM((2, chunks, 3, cycles, block, width), BF16),
        pltpu.VMEM((2, chunks, 3, cycles, block, width), BF16),
        pltpu.VMEM((2, block, tile), BF16),
        pltpu.VMEM((2, 3, block, tile), BF16),
        pltpu.VMEM((2, 3, block, tile), BF16),
        pltpu.VMEM((2, chunks, rows0 // 2, width), F32),
        halves,
        pltpu.VMEM((tiles, padded, tile), F32),
        pltpu.VMEM((tiles, padded, tile), F32),
        pltpu.VMEM((padded, tile), F32),
        pltpu.VMEM((sharers - 1, padded, tile), F32),
        pltpu.SemaphoreType.DMA((chunks,)),
        pltpu.SemaphoreType.DMA((coarse,)),
        pltpu.SemaphoreType.DMA((3,)),
        pltpu.SemaphoreType.DMA((2, 2, chunks, 3)),
        pltpu.SemaphoreType.DMA((2, 2, 3)),
        pltpu.SemaphoreType.DMA((2, steps, 2, chunks)),
        pltpu.SemaphoreType.DMA((2, tiles)),
        pltpu.SemaphoreType.DMA((2, sharers - 1)),
    ]
    anywhere = pl.BlockSpec(memory_space=pl.ANY)
    vmem = pl.BlockSpec(memory_space=pltpu.VMEM)
    harmonics, spectra = pl.pallas_call(
        functools.partial(kernel, cfg),
        out_shape=[
            jax.ShapeDtypeStruct((own * channels, ells), F32),
            jax.ShapeDtypeStruct((pairs, ells // devices), F32),
        ],
        in_specs=[pl.BlockSpec(memory_space=pltpu.SMEM), vmem] + [anywhere] * 5,
        out_specs=[vmem, vmem],
        scratch_shapes=scratch,
        compiler_params=pltpu.CompilerParams(
            vmem_limit_bytes=60 * MIB, collective_id=0, has_side_effects=True
        ),
        cost_estimate=pl.CostEstimate(
            flops=2 * cycles * orders * orders * ells, bytes_accessed=2 * legendre.size, transcendentals=0
        ),
    )(
        owner_table,
        owner_table.reshape(1, orders),
        sky_maps,
        jnp.asarray(first),
        jnp.asarray(high),
        jnp.asarray(low),
        legendre,
    )
    return harmonics.reshape(own, maps, 2, ells), spectra


def solution(mesh):
    return jax.shard_map(
        per_device,
        mesh=mesh,
        in_specs=(P(None, AXES, None), P(AXES, None, None), P()),
        out_specs=(P(AXES, None, None, None), P(None, AXES)),
        check_vma=False,
    )
```

```python
import functools
import math

import jax
import jax.numpy as jnp
import numpy as np
from jax import lax
from jax.experimental import pallas as pl
from jax.experimental.pallas import tpu as pltpu
from jax.sharding import PartitionSpec as P

AXES = ("blk", "grp")
MIB = 1024 * 1024
MESH = pl.DeviceIdType.MESH
BF16 = jnp.bfloat16
F32 = jnp.float32
GROUP = 16
FIRST = (1, 2)
EARLY = 3
WIDTH = 128
AHEAD = 2
LAGS = (2, 3, 3)


def plan_of(bits):
    later = [[EARLY] + [b for b in range(1, bits) if b not in (first, EARLY)] for first in FIRST]
    return later


def flip(me, bits):
    out = me
    for b in bits:
        out = out + (1 - 2 * ((me // (1 << b)) % 2)) * (1 << b)
    return out


def split_bf16(values):
    high = values.astype(BF16)
    low = (values - high.astype(F32)).astype(BF16)
    return high, low


def dot(left, right):
    return jnp.dot(left, right, preferred_element_type=F32)


def dot_t(left, right):
    return lax.dot_general(left, right, (((1,), (1,)), ((), ())), preferred_element_type=F32)


def fourier_tables(pixels, order_count, width):
    coarse = pixels // width
    k1, m1 = np.meshgrid(np.arange(coarse), np.arange(coarse), indexing="ij")
    angle = 2.0 * math.pi * ((k1 * m1) % coarse) / coarse
    first = np.concatenate([np.cos(angle.T), -np.sin(angle.T)], axis=0)
    k2 = np.arange(width)[:, None]
    m = np.arange(order_count)[None, :]
    angle = 2.0 * math.pi * ((k2 * m) % pixels) / pixels
    cosine, sine = np.cos(angle) / math.sqrt(pixels), np.sin(angle) / math.sqrt(pixels)
    second = np.block([[cosine, -sine], [sine, cosine]]).astype(np.float32)
    high = second.astype(jnp.bfloat16)
    low = (second - high.astype(np.float32)).astype(jnp.bfloat16)
    return first.astype(np.float32), high, low


def kernel(
    cfg, owner_smem, owner_ref, sky_hbm, first_hbm, high_hbm, low_hbm, leg_hbm, harm_ref, spec_ref,
    leg_v, sky_v, first_v, high_v, low_v, hot_v, lhs_v, own0, send0, recv0, coef_own, coef_send, coef_recv,
    acc_v, halves, pow_v, pow_recv, pow_mine, pow_pair, load_sem, sky_sem, table_sem,
    sems0, coef_sems, half_sems, pow_sems, pair_sems,
):
    maps, cycles, orders, ells, devices, grp, width = cfg
    bits = devices.bit_length() - 1
    later = plan_of(bits)
    steps = bits - 2
    chunks = ells // width
    channels = 2 * maps
    own = orders // devices
    per_type = own // 2
    block = orders // 8
    rows0 = block * channels
    me = lax.axis_index("blk") * grp + lax.axis_index("grp")
    tile = 128
    tiles = ells // tile
    sharers = tile * devices // ells
    pairs = maps * (maps + 1) // 2

    def at(index):
        return (index // grp, index % grp)

    def bit(b):
        return (me // (1 << b)) % 2

    gather = [[None, flip(me, [0]), flip(me, [FIRST[ty]]), flip(me, [FIRST[ty], 0])] for ty in range(2)]
    near = sorted({(0,)} | {(f,) for f in FIRST} | {(0, f) for f in FIRST} | {(b,) for b in range(1, bits)})

    barrier = pltpu.get_barrier_semaphore()
    for masks in near:
        pl.semaphore_signal(barrier, inc=1, device_id=at(flip(me, masks)), device_id_type=MESH)

    def load(t):
        lanes = pl.ds(pl.multiple_of(t * width, width), width)
        return pltpu.make_async_copy(leg_hbm.at[:, :, lanes], leg_v.at[t], load_sem.at[t])

    def load_start(t, carry):
        load(t).start()
        return carry

    lax.fori_loop(0, chunks, load_start, 0)
    coarse = sky_v.shape[2]

    def sky_load(k):
        lanes = pl.ds(pl.multiple_of(k * tile, tile), tile)
        return pltpu.make_async_copy(sky_hbm.at[:, :, lanes], sky_v.at[:, :, k, :], sky_sem.at[k])

    def sky_start(k, carry):
        sky_load(k).start()
        return carry

    lax.fori_loop(0, coarse, sky_start, 0)
    tables = [
        pltpu.make_async_copy(src, dst, table_sem.at[i])
        for i, (src, dst) in enumerate(((first_hbm, first_v), (high_hbm, high_v), (low_hbm, low_v)))
    ]
    for table in tables:
        table.start()

    j = lax.broadcasted_iota(jnp.int32, (orders, tile), 0)
    half_bit, block_bit = (orders // 2).bit_length() - 1, block.bit_length() - 1
    part = j >> half_bit
    slot = part * per_type + (j & (per_type - 1))

    def place(b, differs):
        mine = bit(b)
        return (mine + differs - 2 * mine * differs) * ((1 << b) * own)

    slot = slot + place(0, (j >> block_bit) & 1)
    for ty in range(2):
        terms = place(FIRST[ty], (j >> (block_bit + 1)) & 1)
        for s, b in enumerate(later[ty]):
            terms = terms + place(b, (j >> (block_bit - s - 1)) & 1)
        slot = slot + jnp.where(part == ty, terms, 0)
    lane = lax.broadcasted_iota(jnp.int32, (orders, tile), 1)
    pick = jnp.concatenate(
        [jnp.where(slot == lane + c * tile, 1.0, 0.0).astype(BF16) for c in range(orders // tile)], axis=1
    )
    table = jnp.where(lax.broadcasted_iota(jnp.int32, (orders, orders), 0) == owner_ref[...], 1.0, 0.0).astype(BF16)
    hot_v[...] = dot_t(pick, table).astype(BF16)

    def gather_copy(ty, t, p):
        return pltpu.make_async_remote_copy(
            src_ref=send0.at[ty, t, p - 1],
            dst_ref=recv0.at[ty, t, p - 1],
            send_sem=sems0.at[0, ty, t, p - 1],
            recv_sem=sems0.at[1, ty, t, p - 1],
            device_id=at(gather[ty][p]),
            device_id_type=MESH,
        )

    def coef_copy(ty, p):
        return pltpu.make_async_remote_copy(
            src_ref=coef_send.at[ty, p - 1],
            dst_ref=coef_recv.at[ty, p - 1],
            send_sem=coef_sems.at[0, ty, p - 1],
            recv_sem=coef_sems.at[1, ty, p - 1],
            device_id=at(gather[ty][p]),
            device_id_type=MESH,
        )

    def half_copy(s, ty, t):
        return pltpu.make_async_remote_copy(
            src_ref=halves[2 * s].at[ty, t],
            dst_ref=halves[2 * s + 1].at[ty, t],
            send_sem=half_sems.at[0, s, ty, t],
            recv_sem=half_sems.at[1, s, ty, t],
            device_id=at(flip(me, [later[ty][s]])),
            device_id_type=MESH,
        )

    def permute(t):
        with jax.named_scope("load"):
            load(t).wait()
        with jax.named_scope("permute"):
            permute_loaded(t)

    def permute_loaded(t):
        together = max(1, 256 // width)
        for r0 in range(0, cycles, together):
            values = jnp.concatenate([leg_v[t, r0 + i] for i in range(together)], axis=1)
            for ty in range(2):
                picked = dot(hot_v[ty * 4 * block : (ty + 1) * 4 * block, :], values).astype(BF16)
                for i in range(together):
                    piece = picked[:, i * width : (i + 1) * width]
                    own0[ty, t, r0 + i] = piece[:block]
                    for p in range(1, 4):
                        send0[ty, t, p - 1, r0 + i] = piece[p * block : (p + 1) * block]
        for p in (2, 3, 1):
            for ty in range(2):
                gather_copy(ty, t, p).start()

    with jax.named_scope("barrier"):
        pl.semaphore_wait(barrier, len(near))
    permute(0)

    def sky_wait(k, carry):
        sky_load(k).wait()
        return carry

    with jax.named_scope("waitsky"):
        lax.fori_loop(0, coarse, sky_wait, 0)
    for table in tables:
        table.wait()
    count = maps * cycles
    columns = 2 * orders
    stages = []
    first = first_v[...]
    for b in range(count):
        stage = jnp.dot(
            first, sky_v[b // cycles, b % cycles], precision=lax.Precision.HIGHEST, preferred_element_type=F32
        )
        stages.append(jnp.concatenate([stage[:coarse], stage[coarse:]], axis=1))
    left_high, left_low = split_bf16(jnp.concatenate(stages, axis=0))
    spectral = []
    span = orders // 2
    for c in range(columns // span):
        picked = slice(c * span, (c + 1) * span)
        full = dot(left_high, high_v[:, picked]) + (dot(left_high, low_v[:, picked]) + dot(left_low, high_v[:, picked]))
        full = full.reshape(count, coarse, span)
        m1 = lax.broadcasted_iota(jnp.int32, (1, coarse, span), 1)
        col = lax.broadcasted_iota(jnp.int32, (1, coarse, span), 2)
        spectral.append(jnp.sum(jnp.where(col % coarse == m1, full, 0.0), axis=1))
    spectral = jnp.concatenate(
        [jnp.concatenate(spectral[:2], axis=1), jnp.concatenate(spectral[2:], axis=1)], axis=0
    ).astype(BF16)
    spectral = jnp.concatenate([spectral, jnp.zeros((tile - 2 * count, orders), BF16)], axis=0)
    coef = dot_t(hot_v[...], spectral).astype(BF16)
    for ty in range(2):
        base = ty * 4 * block
        coef_own[ty] = coef[base : base + block]
        for p in range(1, 4):
            coef_send[ty, p - 1] = coef[base + p * block : base + (p + 1) * block]
    for p in (2, 3, 1):
        for ty in range(2):
            coef_copy(ty, p).start()

    def permute_step(t, carry):
        permute(t)
        return carry

    lax.fori_loop(1, AHEAD + 1, permute_step, 0)

    source = lax.broadcasted_iota(jnp.int32, (tile, cycles * tile), 0)
    target = lax.broadcasted_iota(jnp.int32, (tile, cycles * tile), 1)
    channel = 2 * ((source // cycles) % maps) + source // count
    same = (source % cycles == target // tile) & (channel == target % channels) & (source < 2 * count)
    expand = jnp.where(same, 1.0, 0.0).astype(BF16)
    depth = 4 * cycles * GROUP
    keep = lax.broadcasted_iota(jnp.int32, (depth, tile), 0) % GROUP == (
        lax.broadcasted_iota(jnp.int32, (depth, tile), 1) // channels
    )
    for ty in range(2):
        spread = []
        for p in range(4):
            if p:
                with jax.named_scope("waitcoef"):
                    coef_copy(ty, p).wait_recv()
            values = coef_recv[ty, p - 1] if p else coef_own[ty]
            spread.append(dot(values, expand))
        for g in range(block // GROUP):
            pieces = [
                spread[p][g * GROUP : (g + 1) * GROUP, r * tile : (r + 1) * tile]
                for p in range(4)
                for r in range(cycles)
            ]
            stacked = jnp.where(keep, jnp.concatenate(pieces, axis=0), 0.0)
            lhs_v[ty, g] = stacked.T.astype(BF16)

    groups = block // GROUP
    high_rows = GROUP * channels

    def product(ty, t, g):
        span = slice(g * GROUP, (g + 1) * GROUP)
        parts = [own0[ty, t, :, span, :]] + [recv0[ty, t, p, :, span, :] for p in range(3)]
        right = jnp.concatenate([v.reshape(cycles * GROUP, width) for v in parts], axis=0)
        return dot(lhs_v[ty, g], right)

    def first_step(t):
        for ty in range(2):
            with jax.named_scope("wait0"):
                for p in range(1, 4):
                    gather_copy(ty, t, p).wait_recv()
            for g in range(groups // 2, groups):
                at_row = (g - groups // 2) * high_rows
                halves[0][ty, t, at_row : at_row + high_rows, :] = product(ty, t, g).astype(BF16)
            half_copy(0, ty, t).start()
        for ty in range(2):
            for g in range(groups // 2):
                acc_v[ty, t, g * high_rows : (g + 1) * high_rows, :] = product(ty, t, g)

    def next_step(s, t):
        size = rows0 >> (s + 1)
        for ty in range(2):
            with jax.named_scope(f"wait{s}"):
                half_copy(s - 1, ty, t).wait_recv()
            got = halves[2 * s - 1]
            value = acc_v[ty, t, size : 2 * size, :] + got[ty, t, size:, :].astype(F32)
            halves[2 * s][ty, t] = value.astype(BF16)
            half_copy(s, ty, t).start()
            acc_v[ty, t, :size, :] = acc_v[ty, t, :size, :] + got[ty, t, :size, :].astype(F32)

    def pow_copy(u):
        return pltpu.make_async_remote_copy(
            src_ref=pow_v.at[u],
            dst_ref=pow_recv.at[me // sharers],
            send_sem=pow_sems.at[0, u],
            recv_sem=pow_sems.at[1, me // sharers],
            device_id=at(u * sharers + me % sharers),
            device_id_type=MESH,
        )

    def last_step(t):
        size = rows0 >> steps
        ell = t * width + lax.broadcasted_iota(jnp.int32, (channels, width), 1)
        total = [None] * (maps // 2 + 1)
        lanes = pl.ds(pl.multiple_of(t * width, width), width)
        for ty in range(2):
            with jax.named_scope("waitlast"):
                half_copy(steps - 1, ty, t).wait_recv()
            value = acc_v[ty, t, :size, :] + halves[2 * steps - 1][ty, t].astype(F32)
            for i in range(per_type):
                order = owner_smem[me * own + ty * per_type + i]
                mode = jnp.where(ell >= order, value[i * channels : (i + 1) * channels], 0.0)
                row = (ty * per_type + i) * maps
                for a in range(maps):
                    harm_ref[row + a, :, lanes] = mode[2 * a : 2 * a + 2]
                heavy = mode * jnp.where(order == 0, 1.0, 2.0)
                for k in range(maps // 2 + 1):
                    turned = mode if k == 0 else jnp.concatenate([mode[2 * k :], mode[: 2 * k]], axis=0)
                    term = heavy * turned
                    total[k] = term if total[k] is None else total[k] + term
        rows = []
        for i in range(maps):
            for jj in range(i, maps):
                k, a = (jj - i, i) if jj - i <= maps // 2 else (maps - (jj - i), jj)
                rows.append(total[k][2 * a : 2 * a + 1] + total[k][2 * a + 1 : 2 * a + 2])
        power = jnp.concatenate(rows + [jnp.zeros((pow_v.shape[1] - pairs, width), F32)], axis=0)
        for h in range(width // tile):
            u = t * (width // tile) + h
            pow_v[u] = power[:, h * tile : (h + 1) * tile]

            @pl.when(u != me // sharers)
            def _():
                pow_copy(u).start()

    lags = [0, LAGS[0]]
    for s in range(2, steps):
        lags.append(lags[-1] + LAGS[1])
    end = lags[-1] + LAGS[2]

    def main(t, carry):
        @pl.when((t > 0) & (t + AHEAD < chunks))
        def _():
            permute(t + AHEAD)

        @pl.when(t < chunks)
        def _():
            with jax.named_scope("first"):
                first_step(t)

        for s in range(1, steps):

            @pl.when((t >= lags[s]) & (t < chunks + lags[s]))
            def _():
                with jax.named_scope(f"next{s}"):
                    next_step(s, t - lags[s])

        @pl.when(t >= end)
        def _():
            with jax.named_scope("last"):
                last_step(t - end)

        return carry

    lax.fori_loop(0, chunks + end, main, 0)

    mine = me // sharers
    total = pow_v[mine]
    for u in range(tiles):

        @pl.when(u != mine)
        def _():
            copy = pltpu.make_async_remote_copy(
                src_ref=pow_v.at[u],
                dst_ref=pow_recv.at[u],
                send_sem=pow_sems.at[0, u],
                recv_sem=pow_sems.at[1, u],
                device_id=at(u * sharers + me % sharers),
                device_id_type=MESH,
            )
            with jax.named_scope("waitpow"):
                copy.wait_recv()

    for u in range(tiles):
        total = total + jnp.where(u != mine, pow_recv[u], 0.0)
    pow_mine[...] = total

    def pair_copy(e):
        return pltpu.make_async_remote_copy(
            src_ref=pow_mine,
            dst_ref=pow_pair.at[e - 1],
            send_sem=pair_sems.at[0, e - 1],
            recv_sem=pair_sems.at[1, e - 1],
            device_id=at(mine * sharers + (me + e) % sharers),
            device_id_type=MESH,
        )

    for e in range(1, sharers):
        pair_copy(e).start()
    for e in range(1, sharers):
        with jax.named_scope("waitpair"):
            pair_copy(e).wait_recv()
        total = total + pow_pair[e - 1]
    ell = mine * tile + lax.broadcasted_iota(jnp.int32, total.shape, 1)
    total = total / (2 * ell + 1).astype(F32)
    share = tile // sharers
    turned = total
    for c in range(1, sharers):
        shifted = jnp.concatenate([total[:, c * share :], total[:, : c * share]], axis=1)
        turned = jnp.where(me % sharers == c, shifted, turned)
    spec_ref[...] = turned[:pairs, :share]

    def drain(t, carry):
        for ty in range(2):
            for p in range(1, 4):
                gather_copy(ty, t, p).wait_send()
            for s in range(steps):
                half_copy(s, ty, t).wait_send()
        return carry

    with jax.named_scope("drain"):
        lax.fori_loop(0, chunks, drain, 0)
    for ty in range(2):
        for p in range(1, 4):
            coef_copy(ty, p).wait_send()
    for e in range(1, sharers):
        pair_copy(e).wait_send()
    for u in range(tiles):

        @pl.when(u != mine)
        def _():
            pow_copy(u).wait_send()


def per_device(sky_maps, legendre, owner_table):
    maps, cycles, pixels = sky_maps.shape
    _, orders, ells = legendre.shape
    devices = lax.axis_size(AXES)
    grp = lax.axis_size(AXES[1])
    bits = devices.bit_length() - 1
    steps = bits - 2
    width = WIDTH
    chunks = ells // width
    channels = 2 * maps
    own = orders // devices
    block = orders // 8
    tile = 128
    coarse = pixels // tile
    tiles = ells // tile
    sharers = tile * devices // ells
    pairs = maps * (maps + 1) // 2
    padded = -(-pairs // 8) * 8
    first, high, low = fourier_tables(pixels, orders, tile)
    rows0 = block * channels
    halves = []
    for s in range(steps):
        halves += [pltpu.VMEM((2, chunks, rows0 >> (s + 1), width), BF16)] * 2
    cfg = (maps, cycles, orders, ells, devices, grp, width)
    scratch = [
        pltpu.VMEM((chunks, cycles, orders, width), BF16),
        pltpu.VMEM((maps, cycles, coarse, tile), F32),
        pltpu.VMEM(first.shape, F32),
        pltpu.VMEM(high.shape, BF16),
        pltpu.VMEM(low.shape, BF16),
        pltpu.VMEM((orders, orders), BF16),
        pltpu.VMEM((2, block // GROUP, GROUP * channels, 4 * cycles * GROUP), BF16),
        pltpu.VMEM((2, chunks, cycles, block, width), BF16),
        pltpu.VMEM((2, chunks, 3, cycles, block, width), BF16),
        pltpu.VMEM((2, chunks, 3, cycles, block, width), BF16),
        pltpu.VMEM((2, block, tile), BF16),
        pltpu.VMEM((2, 3, block, tile), BF16),
        pltpu.VMEM((2, 3, block, tile), BF16),
        pltpu.VMEM((2, chunks, rows0 // 2, width), F32),
        halves,
        pltpu.VMEM((tiles, padded, tile), F32),
        pltpu.VMEM((tiles, padded, tile), F32),
        pltpu.VMEM((padded, tile), F32),
        pltpu.VMEM((sharers - 1, padded, tile), F32),
        pltpu.SemaphoreType.DMA((chunks,)),
        pltpu.SemaphoreType.DMA((coarse,)),
        pltpu.SemaphoreType.DMA((3,)),
        pltpu.SemaphoreType.DMA((2, 2, chunks, 3)),
        pltpu.SemaphoreType.DMA((2, 2, 3)),
        pltpu.SemaphoreType.DMA((2, steps, 2, chunks)),
        pltpu.SemaphoreType.DMA((2, tiles)),
        pltpu.SemaphoreType.DMA((2, sharers - 1)),
    ]
    anywhere = pl.BlockSpec(memory_space=pl.ANY)
    vmem = pl.BlockSpec(memory_space=pltpu.VMEM)
    harmonics, spectra = pl.pallas_call(
        functools.partial(kernel, cfg),
        out_shape=[
            jax.ShapeDtypeStruct((own * maps, 2, ells), F32),
            jax.ShapeDtypeStruct((pairs, ells // devices), F32),
        ],
        in_specs=[pl.BlockSpec(memory_space=pltpu.SMEM), vmem] + [anywhere] * 5,
        out_specs=[vmem, vmem],
        scratch_shapes=scratch,
        compiler_params=pltpu.CompilerParams(
            vmem_limit_bytes=60 * MIB, collective_id=0, has_side_effects=True
        ),
        cost_estimate=pl.CostEstimate(
            flops=2 * cycles * orders * orders * ells, bytes_accessed=2 * legendre.size, transcendentals=0
        ),
    )(
        owner_table,
        owner_table.reshape(1, orders),
        sky_maps,
        jnp.asarray(first),
        jnp.asarray(high),
        jnp.asarray(low),
        legendre,
    )
    return harmonics.reshape(own, maps, 2, ells), spectra


def solution(mesh):
    return jax.shard_map(
        per_device,
        mesh=mesh,
        in_specs=(P(None, AXES, None), P(AXES, None, None), P()),
        out_specs=(P(AXES, None, None, None), P(None, AXES)),
        check_vma=False,
    )
```

```python
import functools
import math

import jax
import jax.numpy as jnp
import numpy as np
from jax import lax
from jax.experimental import pallas as pl
from jax.experimental.pallas import tpu as pltpu
from jax.sharding import PartitionSpec as P

AXES = ("blk", "grp")
MIB = 1024 * 1024
MESH = pl.DeviceIdType.MESH
BF16 = jnp.bfloat16
F32 = jnp.float32
GROUP = 16
FIRST = (1, 2)
EARLY = 3
WIDTH = 128
AHEAD = 3
SWAPPED = 1
SLOTS = 10
LAGS = (3, 3, 4)


def plan_of(bits):
    later = [[EARLY] + [b for b in range(1, bits) if b not in (first, EARLY)] for first in FIRST]
    return later


def flip(me, bits):
    out = me
    for b in bits:
        out = out + (1 - 2 * ((me // (1 << b)) % 2)) * (1 << b)
    return out


def split_bf16(values):
    high = values.astype(BF16)
    low = (values - high.astype(F32)).astype(BF16)
    return high, low


def dot(left, right):
    return jnp.dot(left, right, preferred_element_type=F32)


def dot_t(left, right):
    return lax.dot_general(left, right, (((1,), (1,)), ((), ())), preferred_element_type=F32)


def fourier_tables(pixels, order_count, width):
    coarse = pixels // width
    k1, m1 = np.meshgrid(np.arange(coarse), np.arange(coarse), indexing="ij")
    angle = 2.0 * math.pi * ((k1 * m1) % coarse) / coarse
    first = np.concatenate([np.cos(angle.T), -np.sin(angle.T)], axis=0)
    k2 = np.arange(width)[:, None]
    m = np.arange(order_count)[None, :]
    angle = 2.0 * math.pi * ((k2 * m) % pixels) / pixels
    cosine, sine = np.cos(angle) / math.sqrt(pixels), np.sin(angle) / math.sqrt(pixels)
    second = np.block([[cosine, -sine], [sine, cosine]]).astype(np.float32)
    high = second.astype(jnp.bfloat16)
    low = (second - high.astype(np.float32)).astype(jnp.bfloat16)
    return first.astype(np.float32), high, low


def kernel(
    cfg, owner_smem, owner_ref, sky_hbm, first_hbm, high_hbm, low_hbm, leg_hbm, harm_ref, spec_ref,
    leg_v, sky_v, first_v, high_v, low_v, hot_v, lhs_v, own0, send0, recv0, coef_own, coef_send, coef_recv,
    acc_v, halves, harm_v, pow_v, pow_recv, pow_mine, pow_pair, load_sem, sky_sem, table_sem,
    sent_sems, sems0, coef_sems, half_sems, harm_sem, pow_sem, pair_sems,
):
    maps, cycles, orders, ells, devices, grp, width = cfg
    bits = devices.bit_length() - 1
    later = plan_of(bits)
    steps = bits - 2
    chunks = ells // width
    channels = 2 * maps
    own = orders // devices
    per_type = own // 2
    block = orders // 8
    rows0 = block * channels
    me = lax.axis_index("blk") * grp + lax.axis_index("grp")
    tile = 128
    tiles = ells // tile
    sharers = tile * devices // ells
    pairs = maps * (maps + 1) // 2

    def at(index):
        return (index // grp, index % grp)

    def bit(b):
        return (me // (1 << b)) % 2

    gather = [[None, flip(me, [0]), flip(me, [FIRST[ty]]), flip(me, [FIRST[ty], 0])] for ty in range(2)]
    near = sorted({(0,)} | {(f,) for f in FIRST} | {(0, f) for f in FIRST} | {(b,) for b in range(1, bits)})

    scope = jax.named_scope
    barrier = pltpu.get_barrier_semaphore()
    for masks in near:
        pl.semaphore_signal(barrier, inc=1, device_id=at(flip(me, masks)), device_id_type=MESH)

    def load(t):
        lanes = pl.ds(pl.multiple_of(t * width, width), width)
        return pltpu.make_async_copy(leg_hbm.at[:, :, lanes], leg_v.at[t], load_sem.at[t % 4])

    def load_start(t, carry):
        load(t).start()
        return carry

    with scope("startload"):
        lax.fori_loop(0, 4, load_start, 0)
    coarse = sky_v.shape[2]

    def sky_load(k):
        lanes = pl.ds(pl.multiple_of(k * tile, tile), tile)
        return pltpu.make_async_copy(sky_hbm.at[:, :, lanes], sky_v.at[:, :, k, :], sky_sem)

    def sky_start(k, carry):
        sky_load(k).start()
        return carry

    with scope("startsky"):
        lax.fori_loop(0, coarse, sky_start, 0)
    tables = [
        pltpu.make_async_copy(src, dst, table_sem.at[i])
        for i, (src, dst) in enumerate(((first_hbm, first_v), (high_hbm, high_v), (low_hbm, low_v)))
    ]
    for table in tables:
        table.start()

    j = lax.broadcasted_iota(jnp.int32, (orders, tile), 0)
    half_bit, block_bit = (orders // 2).bit_length() - 1, block.bit_length() - 1
    part = j >> half_bit
    slot = part * per_type + (j & (per_type - 1))

    def place(b, differs):
        mine = bit(b)
        return (mine + differs - 2 * mine * differs) * ((1 << b) * own)

    slot = slot + place(0, (j >> block_bit) & 1)
    for ty in range(2):
        terms = place(FIRST[ty], (j >> (block_bit + 1)) & 1)
        for s, b in enumerate(later[ty]):
            terms = terms + place(b, (j >> (block_bit - s - 1)) & 1)
        slot = slot + jnp.where(part == ty, terms, 0)
    lane = lax.broadcasted_iota(jnp.int32, (orders, tile), 1)
    pick = jnp.concatenate(
        [jnp.where(slot == lane + c * tile, 1.0, 0.0).astype(BF16) for c in range(orders // tile)], axis=1
    )
    table = jnp.where(lax.broadcasted_iota(jnp.int32, (orders, orders), 0) == owner_ref[...], 1.0, 0.0).astype(BF16)
    hot_v[...] = dot_t(pick, table).astype(BF16)

    def whole(ref, sem):
        return pltpu.make_async_copy(ref, ref, sem)

    def gather_copy(ty, t, p):
        return pltpu.make_async_remote_copy(
            src_ref=send0.at[ty, t, p - 1],
            dst_ref=recv0.at[ty, t, p - 1],
            send_sem=sent_sems.at[0],
            recv_sem=sems0.at[t % SLOTS, ty],
            device_id=at(gather[ty][p]),
            device_id_type=MESH,
        )

    def coef_copy(ty, p):
        return pltpu.make_async_remote_copy(
            src_ref=coef_send.at[ty, p - 1],
            dst_ref=coef_recv.at[ty, p - 1],
            send_sem=sent_sems.at[1],
            recv_sem=coef_sems.at[ty],
            device_id=at(gather[ty][p]),
            device_id_type=MESH,
        )

    swap_from = chunks - SWAPPED
    groups = block // GROUP

    def half_copy(s, ty, t):
        partner = flip(me, [later[ty][s]])
        if s < 2:
            partner = jnp.where(t < swap_from, partner, flip(me, [later[ty][1 - s]]))
        return pltpu.make_async_remote_copy(
            src_ref=halves[2 * s].at[ty, t],
            dst_ref=halves[2 * s + 1].at[ty, t],
            send_sem=sent_sems.at[2 + s],
            recv_sem=half_sems.at[s, t % SLOTS, ty],
            device_id=at(partner),
            device_id_type=MESH,
        )

    def permute(t):
        with jax.named_scope("load"):
            load(t).wait()
        with jax.named_scope("permute"):
            permute_loaded(t)

        @pl.when(t + 4 < chunks)
        def _():
            load(t + 4).start()

    def permute_loaded(t):
        together = max(1, 256 // width)
        for r0 in range(0, cycles, together):
            values = jnp.concatenate([leg_v[t, r0 + i] for i in range(together)], axis=1)
            for ty in range(2):
                picked = dot(hot_v[ty * 4 * block : (ty + 1) * 4 * block, :], values).astype(BF16)
                for i in range(together):
                    piece = picked[:, i * width : (i + 1) * width]
                    own0[ty, t, r0 + i] = piece[:block]
                    for p in range(1, 4):
                        send0[ty, t, p - 1, r0 + i] = piece[p * block : (p + 1) * block]
        for p in (2, 3, 1):
            for ty in range(2):
                gather_copy(ty, t, p).start()

    with jax.named_scope("barrier"):
        pl.semaphore_wait(barrier, len(near))
    permute(0)

    with jax.named_scope("waitsky"):
        whole(sky_v, sky_sem).wait()
    for table in tables:
        table.wait()
    count = maps * cycles
    columns = 2 * orders
    stages = []
    first = first_v[...]
    for b in range(count):
        stage = jnp.dot(
            first, sky_v[b // cycles, b % cycles], precision=lax.Precision.HIGHEST, preferred_element_type=F32
        )
        stages.append(jnp.concatenate([stage[:coarse], stage[coarse:]], axis=1))
    left_high, left_low = split_bf16(jnp.concatenate(stages, axis=0))
    spectral = []
    span = orders // 2
    for c in range(columns // span):
        picked = slice(c * span, (c + 1) * span)
        full = dot(left_high, high_v[:, picked]) + (dot(left_high, low_v[:, picked]) + dot(left_low, high_v[:, picked]))
        full = full.reshape(count, coarse, span)
        m1 = lax.broadcasted_iota(jnp.int32, (1, coarse, span), 1)
        col = lax.broadcasted_iota(jnp.int32, (1, coarse, span), 2)
        spectral.append(jnp.sum(jnp.where(col % coarse == m1, full, 0.0), axis=1))
    spectral = jnp.concatenate(
        [jnp.concatenate(spectral[:2], axis=1), jnp.concatenate(spectral[2:], axis=1)], axis=0
    ).astype(BF16)
    spectral = jnp.concatenate([spectral, jnp.zeros((tile - 2 * count, orders), BF16)], axis=0)
    coef = dot_t(hot_v[...], spectral).astype(BF16)
    for ty in range(2):
        base = ty * 4 * block
        coef_own[ty] = coef[base : base + block]
        for p in range(1, 4):
            coef_send[ty, p - 1] = coef[base + p * block : base + (p + 1) * block]
    for p in (2, 3, 1):
        for ty in range(2):
            coef_copy(ty, p).start()

    def permute_step(t, carry):
        permute(t)
        return carry

    lax.fori_loop(1, AHEAD + 1, permute_step, 0)

    source = lax.broadcasted_iota(jnp.int32, (tile, cycles * tile), 0)
    target = lax.broadcasted_iota(jnp.int32, (tile, cycles * tile), 1)
    channel = 2 * ((source // cycles) % maps) + source // count
    same = (source % cycles == target // tile) & (channel == target % channels) & (source < 2 * count)
    expand = jnp.where(same, 1.0, 0.0).astype(BF16)
    depth = 4 * cycles * GROUP
    keep = lax.broadcasted_iota(jnp.int32, (depth, tile), 0) % GROUP == (
        lax.broadcasted_iota(jnp.int32, (depth, tile), 1) // channels
    )
    for ty in range(2):
        spread = []
        with jax.named_scope("waitcoef"):
            whole(coef_recv.at[ty], coef_sems.at[ty]).wait()
        for p in range(4):
            values = coef_recv[ty, p - 1] if p else coef_own[ty]
            spread.append(dot(values, expand))
        for g in range(block // GROUP):
            pieces = [
                spread[p][g * GROUP : (g + 1) * GROUP, r * tile : (r + 1) * tile]
                for p in range(4)
                for r in range(cycles)
            ]
            stacked = jnp.where(keep, jnp.concatenate(pieces, axis=0), 0.0)
            lhs_v[ty, g] = stacked.T.astype(BF16)

    high_rows = GROUP * channels

    def product(ty, t, g):
        span = slice(g * GROUP, (g + 1) * GROUP)
        parts = [own0[ty, t, :, span, :]] + [recv0[ty, t, p, :, span, :] for p in range(3)]
        right = jnp.concatenate([v.reshape(cycles * GROUP, width) for v in parts], axis=0)
        return dot(lhs_v[ty, g], right)

    def first_step(t, sent, kept):
        for ty in range(2):
            with jax.named_scope("wait0"):
                whole(recv0.at[ty, t], sems0.at[t % SLOTS, ty]).wait()
            for i, g in enumerate(sent):
                halves[0][ty, t, i * high_rows : (i + 1) * high_rows, :] = product(ty, t, g).astype(BF16)
            half_copy(0, ty, t).start()
        for ty in range(2):
            for i, g in enumerate(kept):
                acc_v[ty, t, i * high_rows : (i + 1) * high_rows, :] = product(ty, t, g)

    def next_step(s, t):
        size = rows0 >> (s + 1)
        for ty in range(2):
            with jax.named_scope(f"wait{s}"):
                half_copy(s - 1, ty, t).wait_recv()
            got = halves[2 * s - 1]
            value = acc_v[ty, t, size : 2 * size, :] + got[ty, t, size:, :].astype(F32)
            halves[2 * s][ty, t] = value.astype(BF16)
            half_copy(s, ty, t).start()
            acc_v[ty, t, :size, :] = acc_v[ty, t, :size, :] + got[ty, t, :size, :].astype(F32)

    def pow_copy(u):
        return pltpu.make_async_remote_copy(
            src_ref=pow_v.at[u],
            dst_ref=pow_recv.at[me // sharers],
            send_sem=sent_sems.at[2 + steps],
            recv_sem=pow_sem,
            device_id=at(u * sharers + me % sharers),
            device_id_type=MESH,
        )

    def harm_copy(t):
        lanes = pl.ds(pl.multiple_of(t * width, width), width)
        return pltpu.make_async_copy(harm_v.at[t], harm_ref.at[:, :, lanes], harm_sem)

    def last_step(t):
        size = rows0 >> steps
        ell = t * width + lax.broadcasted_iota(jnp.int32, (channels, width), 1)
        total = [None] * (maps // 2 + 1)
        for ty in range(2):
            with jax.named_scope("waitlast"):
                half_copy(steps - 1, ty, t).wait_recv()
            value = acc_v[ty, t, :size, :] + halves[2 * steps - 1][ty, t].astype(F32)
            for i in range(per_type):
                order = owner_smem[me * own + ty * per_type + i]
                mode = jnp.where(ell >= order, value[i * channels : (i + 1) * channels], 0.0)
                row = (ty * per_type + i) * maps
                for a in range(maps):
                    harm_v[t, row + a] = mode[2 * a : 2 * a + 2]
                heavy = mode * jnp.where(order == 0, 1.0, 2.0)
                for k in range(maps // 2 + 1):
                    turned = mode if k == 0 else jnp.concatenate([mode[2 * k :], mode[: 2 * k]], axis=0)
                    term = heavy * turned
                    total[k] = term if total[k] is None else total[k] + term
        harm_copy(t).start()
        rows = []
        for i in range(maps):
            for jj in range(i, maps):
                k, a = (jj - i, i) if jj - i <= maps // 2 else (maps - (jj - i), jj)
                rows.append(total[k][2 * a : 2 * a + 1] + total[k][2 * a + 1 : 2 * a + 2])
        power = jnp.concatenate(rows + [jnp.zeros((pow_v.shape[1] - pairs, width), F32)], axis=0)
        for h in range(width // tile):
            u = t * (width // tile) + h
            pow_v[u] = power[:, h * tile : (h + 1) * tile]

            @pl.when(u != me // sharers)
            def _():
                pow_copy(u).start()

    lags = [0, LAGS[0]]
    for s in range(2, steps):
        lags.append(lags[-1] + LAGS[1])
    end = lags[-1] + LAGS[2]

    def main(t, carry):
        @pl.when((t > 0) & (t + AHEAD < chunks))
        def _():
            permute(t + AHEAD)

        @pl.when(t < swap_from)
        def _():
            with jax.named_scope("first"):
                first_step(t, (2, 3), (0, 1))

        @pl.when((t >= swap_from) & (t < chunks))
        def _():
            with jax.named_scope("first"):
                first_step(t, (1, 3), (0, 2))

        for s in range(1, steps):

            @pl.when((t >= lags[s]) & (t < chunks + lags[s]))
            def _():
                with jax.named_scope(f"next{s}"):
                    next_step(s, t - lags[s])

        @pl.when(t >= end)
        def _():
            with jax.named_scope("last"):
                last_step(t - end)

        return carry

    lax.fori_loop(0, chunks + end, main, 0)

    mine = me // sharers
    total = pow_v[mine]
    with scope("waitpow"):
        whole(pow_recv.at[: tiles - 1], pow_sem).wait()
    for u in range(tiles):
        total = total + jnp.where(u != mine, pow_recv[u], 0.0)
    pow_mine[...] = total

    def pair_copy(e):
        return pltpu.make_async_remote_copy(
            src_ref=pow_mine,
            dst_ref=pow_pair.at[e - 1],
            send_sem=pair_sems.at[0, e - 1],
            recv_sem=pair_sems.at[1, e - 1],
            device_id=at(mine * sharers + (me + e) % sharers),
            device_id_type=MESH,
        )

    for e in range(1, sharers):
        pair_copy(e).start()
    for e in range(1, sharers):
        with jax.named_scope("waitpair"):
            pair_copy(e).wait_recv()
        total = total + pow_pair[e - 1]
    ell = mine * tile + lax.broadcasted_iota(jnp.int32, total.shape, 1)
    total = total / (2 * ell + 1).astype(F32)
    share = tile // sharers
    turned = total
    for c in range(1, sharers):
        shifted = jnp.concatenate([total[:, c * share :], total[:, : c * share]], axis=1)
        turned = jnp.where(me % sharers == c, shifted, turned)
    spec_ref[...] = turned[:pairs, :share]

    with jax.named_scope("drain"):
        whole(harm_v, harm_sem).wait()
        whole(send0, sent_sems.at[0]).wait()
        whole(coef_send, sent_sems.at[1]).wait()
        for s in range(steps):
            whole(halves[2 * s], sent_sems.at[2 + s]).wait()
    for e in range(1, sharers):
        pair_copy(e).wait_send()
    whole(pow_v.at[: tiles - 1], sent_sems.at[2 + steps]).wait()


def hand_over_body(parts, large_ref, small_ref, large_out, small_out, large_v, small_v, sems, small_sems):
    rows = large_v.shape[0] // parts
    ins, outs = [], []
    for c in range(parts):
        picked = slice(c * rows, (c + 1) * rows)
        ins.append(pltpu.make_async_copy(large_ref.at[picked], large_v.at[picked], sems.at[0, c]))
        outs.append(pltpu.make_async_copy(large_v.at[picked], large_out.at[picked], sems.at[1, c]))
    ins.append(pltpu.make_async_copy(small_ref, small_v, small_sems.at[0]))
    outs.append(pltpu.make_async_copy(small_v, small_out, small_sems.at[1]))
    for copy in ins:
        copy.start()
    for got, put in zip(ins, outs):
        got.wait()
        put.start()
    for copy in outs:
        copy.wait()


def hand_over(large, small):
    parts = 4
    anywhere = pl.BlockSpec(memory_space=pl.ANY)
    return pl.pallas_call(
        functools.partial(hand_over_body, parts),
        out_shape=[jax.ShapeDtypeStruct(large.shape, large.dtype), jax.ShapeDtypeStruct(small.shape, small.dtype)],
        in_specs=[anywhere] * 2,
        out_specs=[anywhere] * 2,
        scratch_shapes=[
            pltpu.VMEM(large.shape, large.dtype),
            pltpu.VMEM(small.shape, small.dtype),
            pltpu.SemaphoreType.DMA((2, parts)),
            pltpu.SemaphoreType.DMA((2,)),
        ],
        cost_estimate=pl.CostEstimate(flops=large.size, bytes_accessed=8 * large.size, transcendentals=0),
    )(large, small)


def per_device(sky_maps, legendre, owner_table):
    maps, cycles, pixels = sky_maps.shape
    _, orders, ells = legendre.shape
    devices = lax.axis_size(AXES)
    grp = lax.axis_size(AXES[1])
    bits = devices.bit_length() - 1
    steps = bits - 2
    width = WIDTH
    chunks = ells // width
    channels = 2 * maps
    own = orders // devices
    block = orders // 8
    tile = 128
    coarse = pixels // tile
    tiles = ells // tile
    sharers = tile * devices // ells
    pairs = maps * (maps + 1) // 2
    padded = -(-pairs // 8) * 8
    first, high, low = fourier_tables(pixels, orders, tile)
    rows0 = block * channels
    halves = []
    for s in range(steps):
        halves += [pltpu.VMEM((2, chunks, rows0 >> (s + 1), width), BF16)] * 2
    cfg = (maps, cycles, orders, ells, devices, grp, width)
    scratch = [
        pltpu.VMEM((chunks, cycles, orders, width), BF16),
        pltpu.VMEM((maps, cycles, coarse, tile), F32),
        pltpu.VMEM(first.shape, F32),
        pltpu.VMEM(high.shape, BF16),
        pltpu.VMEM(low.shape, BF16),
        pltpu.VMEM((orders, orders), BF16),
        pltpu.VMEM((2, block // GROUP, GROUP * channels, 4 * cycles * GROUP), BF16),
        pltpu.VMEM((2, chunks, cycles, block, width), BF16),
        pltpu.VMEM((2, chunks, 3, cycles, block, width), BF16),
        pltpu.VMEM((2, chunks, 3, cycles, block, width), BF16),
        pltpu.VMEM((2, block, tile), BF16),
        pltpu.VMEM((2, 3, block, tile), BF16),
        pltpu.VMEM((2, 3, block, tile), BF16),
        pltpu.VMEM((2, chunks, rows0 // 2, width), F32),
        halves,
        pltpu.VMEM((chunks, own * maps, 2, width), F32),
        pltpu.VMEM((tiles, padded, tile), F32),
        pltpu.VMEM((tiles, padded, tile), F32),
        pltpu.VMEM((padded, tile), F32),
        pltpu.VMEM((sharers - 1, padded, tile), F32),
        pltpu.SemaphoreType.DMA((4,)),
        pltpu.SemaphoreType.DMA,
        pltpu.SemaphoreType.DMA((3,)),
        pltpu.SemaphoreType.DMA((3 + steps,)),
        pltpu.SemaphoreType.DMA((SLOTS, 2)),
        pltpu.SemaphoreType.DMA((2,)),
        pltpu.SemaphoreType.DMA((steps, SLOTS, 2)),
        pltpu.SemaphoreType.DMA,
        pltpu.SemaphoreType.DMA,
        pltpu.SemaphoreType.DMA((2, sharers - 1)),
    ]
    anywhere = pl.BlockSpec(memory_space=pl.ANY)
    vmem = pl.BlockSpec(memory_space=pltpu.VMEM)
    harmonics, spectra = pl.pallas_call(
        functools.partial(kernel, cfg),
        out_shape=[
            jax.ShapeDtypeStruct((own * maps, 2, ells), F32),
            jax.ShapeDtypeStruct((pairs, ells // devices), F32),
        ],
        in_specs=[pl.BlockSpec(memory_space=pltpu.SMEM), vmem] + [anywhere] * 5,
        out_specs=[anywhere, vmem],
        scratch_shapes=scratch,
        compiler_params=pltpu.CompilerParams(
            vmem_limit_bytes=60 * MIB, collective_id=0, has_side_effects=True
        ),
        cost_estimate=pl.CostEstimate(
            flops=2 * cycles * orders * orders * ells, bytes_accessed=2 * legendre.size, transcendentals=0
        ),
    )(
        owner_table,
        owner_table.reshape(1, orders),
        sky_maps,
        jnp.asarray(first),
        jnp.asarray(high),
        jnp.asarray(low),
        legendre,
    )
    harmonics, spectra = hand_over(harmonics, spectra)
    return harmonics.reshape(own, maps, 2, ells), spectra


def solution(mesh):
    return jax.shard_map(
        per_device,
        mesh=mesh,
        in_specs=(P(None, AXES, None), P(AXES, None, None), P()),
        out_specs=(P(AXES, None, None, None), P(None, AXES)),
        check_vma=False,
    )
```

```python
import functools
import math

import jax
import jax.numpy as jnp
import numpy as np
from jax import lax
from jax.experimental import pallas as pl
from jax.experimental.pallas import tpu as pltpu
from jax.sharding import PartitionSpec as P

AXES = ("blk", "grp")
MIB = 1024 * 1024
MESH = pl.DeviceIdType.MESH
BF16 = jnp.bfloat16
F32 = jnp.float32
GROUP = 16
FIRST = (1, 2)
EARLY = 3
WIDTH = 128
AHEAD = 3
SWAPPED = 2
SLOTS = 8
LAGS = (2, 2, 3)


def plan_of(bits):
    later = [[EARLY] + [b for b in range(1, bits) if b not in (first, EARLY)] for first in FIRST]
    return later


def flip(me, bits):
    out = me
    for b in bits:
        out = out + (1 - 2 * ((me // (1 << b)) % 2)) * (1 << b)
    return out


def split_bf16(values):
    high = values.astype(BF16)
    low = (values - high.astype(F32)).astype(BF16)
    return high, low


def dot(left, right):
    return jnp.dot(left, right, preferred_element_type=F32)


def dot_t(left, right):
    return lax.dot_general(left, right, (((1,), (1,)), ((), ())), preferred_element_type=F32)


def fourier_tables(pixels, order_count, width):
    coarse = pixels // width
    k1, m1 = np.meshgrid(np.arange(coarse), np.arange(coarse), indexing="ij")
    angle = 2.0 * math.pi * ((k1 * m1) % coarse) / coarse
    first = np.concatenate([np.cos(angle.T), -np.sin(angle.T)], axis=0)
    k2 = np.arange(width)[:, None]
    m = np.arange(order_count)[None, :]
    angle = 2.0 * math.pi * ((k2 * m) % pixels) / pixels
    cosine, sine = np.cos(angle) / math.sqrt(pixels), np.sin(angle) / math.sqrt(pixels)
    second = np.block([[cosine, -sine], [sine, cosine]]).astype(np.float32)
    high = second.astype(jnp.bfloat16)
    low = (second - high.astype(np.float32)).astype(jnp.bfloat16)
    return first.astype(np.float32), high, low


def kernel(
    cfg, owner_hbm, owner_row_hbm, sky_hbm, first_hbm, high_hbm, low_hbm, leg_hbm, harm_ref, spec_ref,
    owner_smem, owner_ref, leg_v, sky_v, first_v, high_v, low_v, hot_v, lhs_v, own0, send0, recv0, coef_own, coef_send, coef_recv,
    acc_v, halves, pow_v, pow_recv, pow_mine, pow_pair, load_sem, sky_sem, table_sem,
    sent_sems, sems0, coef_sems, half_sems, pow_sem, pair_sems,
):
    maps, cycles, orders, ells, devices, grp, width = cfg
    bits = devices.bit_length() - 1
    later = plan_of(bits)
    steps = bits - 2
    chunks = ells // width
    channels = 2 * maps
    own = orders // devices
    per_type = own // 2
    block = orders // 8
    rows0 = block * channels
    me = lax.axis_index("blk") * grp + lax.axis_index("grp")
    tile = 128
    tiles = ells // tile
    sharers = tile * devices // ells
    pairs = maps * (maps + 1) // 2

    def at(index):
        return (index // grp, index % grp)

    def bit(b):
        return (me // (1 << b)) % 2

    gather = [[None, flip(me, [0]), flip(me, [FIRST[ty]]), flip(me, [FIRST[ty], 0])] for ty in range(2)]
    near = sorted({(0,)} | {(f,) for f in FIRST} | {(0, f) for f in FIRST} | {(b,) for b in range(1, bits)})

    scope = jax.named_scope
    row_load = pltpu.make_async_copy(owner_row_hbm, owner_ref, table_sem.at[3])
    row_load.start()
    barrier = pltpu.get_barrier_semaphore()
    for masks in near:
        pl.semaphore_signal(barrier, inc=1, device_id=at(flip(me, masks)), device_id_type=MESH)

    def load(t):
        lanes = pl.ds(pl.multiple_of(t * width, width), width)
        return pltpu.make_async_copy(leg_hbm.at[:, :, lanes], leg_v.at[t], load_sem.at[t % 4])

    def load_start(t, carry):
        load(t).start()
        return carry

    with scope("startload"):
        lax.fori_loop(0, 4, load_start, 0)
    coarse = sky_v.shape[2]

    def sky_load(k):
        lanes = pl.ds(k * tile, tile)
        return pltpu.make_async_copy(sky_hbm.at[:, :, lanes], sky_v.at[:, :, k, :], sky_sem)

    for k in range(coarse):
        sky_load(k).start()
    tables = [
        pltpu.make_async_copy(src, dst, table_sem.at[i])
        for i, (src, dst) in enumerate(((first_hbm, first_v), (high_hbm, high_v), (low_hbm, low_v)))
    ]
    for table in tables:
        table.start()


    j = lax.broadcasted_iota(jnp.int32, (orders, tile), 0)
    half_bit, block_bit = (orders // 2).bit_length() - 1, block.bit_length() - 1
    part = j >> half_bit
    slot = part * per_type + (j & (per_type - 1))

    def place(b, differs):
        mine = bit(b)
        return (mine + differs - 2 * mine * differs) * ((1 << b) * own)

    slot = slot + place(0, (j >> block_bit) & 1)
    for ty in range(2):
        terms = place(FIRST[ty], (j >> (block_bit + 1)) & 1)
        for s, b in enumerate(later[ty]):
            terms = terms + place(b, (j >> (block_bit - s - 1)) & 1)
        slot = slot + jnp.where(part == ty, terms, 0)
    lane = lax.broadcasted_iota(jnp.int32, (orders, tile), 1)
    pick = jnp.concatenate(
        [jnp.where(slot == lane + c * tile, 1.0, 0.0).astype(BF16) for c in range(orders // tile)], axis=1
    )
    row_load.wait()
    table = jnp.where(lax.broadcasted_iota(jnp.int32, (orders, orders), 0) == owner_ref[...], 1.0, 0.0).astype(BF16)
    hot_v[...] = dot_t(pick, table).astype(BF16)

    def whole(ref, sem):
        return pltpu.make_async_copy(ref, ref, sem)

    def gather_copy(ty, t, p):
        return pltpu.make_async_remote_copy(
            src_ref=send0.at[ty, t, p - 1],
            dst_ref=recv0.at[ty, t, p - 1],
            send_sem=sent_sems.at[0],
            recv_sem=sems0.at[t % SLOTS, ty],
            device_id=at(gather[ty][p]),
            device_id_type=MESH,
        )

    def coef_copy(ty, p):
        return pltpu.make_async_remote_copy(
            src_ref=coef_send.at[ty, p - 1],
            dst_ref=coef_recv.at[ty, p - 1],
            send_sem=sent_sems.at[1],
            recv_sem=coef_sems.at[ty],
            device_id=at(gather[ty][p]),
            device_id_type=MESH,
        )

    swap_from = chunks - SWAPPED
    groups = block // GROUP

    def half_copy(s, ty, t):
        partner = flip(me, [later[ty][s]])
        if s < 2:
            partner = jnp.where(t < swap_from, partner, flip(me, [later[ty][1 - s]]))
        return pltpu.make_async_remote_copy(
            src_ref=halves[2 * s].at[ty, t],
            dst_ref=halves[2 * s + 1].at[ty, t],
            send_sem=sent_sems.at[2 + s],
            recv_sem=half_sems.at[s, t % SLOTS, ty],
            device_id=at(partner),
            device_id_type=MESH,
        )

    def permute(t):
        with jax.named_scope("load"):
            load(t).wait()
        with jax.named_scope("permute"):
            permute_loaded(t)

        @pl.when(t + 4 < chunks)
        def _():
            load(t + 4).start()

    def permute_loaded(t):
        together = max(1, 256 // width)
        for r0 in range(0, cycles, together):
            values = jnp.concatenate([leg_v[t, r0 + i] for i in range(together)], axis=1)
            for ty in range(2):
                picked = dot(hot_v[ty * 4 * block : (ty + 1) * 4 * block, :], values).astype(BF16)
                for i in range(together):
                    piece = picked[:, i * width : (i + 1) * width]
                    own0[ty, t, r0 + i] = piece[:block]
                    for p in range(1, 4):
                        send0[ty, t, p - 1, r0 + i] = piece[p * block : (p + 1) * block]
        for p in (2, 3, 1):
            for ty in range(2):
                gather_copy(ty, t, p).start()

    with jax.named_scope("barrier"):
        pl.semaphore_wait(barrier, len(near))
    permute(0)
    order_load = pltpu.make_async_copy(owner_hbm, owner_smem, table_sem.at[4])
    order_load.start()

    with jax.named_scope("waitsky"):
        whole(sky_v, sky_sem).wait()
    for table in tables:
        table.wait()
    count = maps * cycles
    columns = 2 * orders
    stages = []
    first = first_v[...]
    for b in range(count):
        stage = jnp.dot(
            first, sky_v[b // cycles, b % cycles], precision=lax.Precision.HIGHEST, preferred_element_type=F32
        )
        stages.append(jnp.concatenate([stage[:coarse], stage[coarse:]], axis=1))
    left_high, left_low = split_bf16(jnp.concatenate(stages, axis=0))
    spectral = []
    span = orders // 2
    for c in range(columns // span):
        picked = slice(c * span, (c + 1) * span)
        full = dot(left_high, high_v[:, picked]) + (dot(left_high, low_v[:, picked]) + dot(left_low, high_v[:, picked]))
        full = full.reshape(count, coarse, span)
        m1 = lax.broadcasted_iota(jnp.int32, (1, coarse, span), 1)
        col = lax.broadcasted_iota(jnp.int32, (1, coarse, span), 2)
        spectral.append(jnp.sum(jnp.where(col % coarse == m1, full, 0.0), axis=1))
    spectral = jnp.concatenate(
        [jnp.concatenate(spectral[:2], axis=1), jnp.concatenate(spectral[2:], axis=1)], axis=0
    ).astype(BF16)
    spectral = jnp.concatenate([spectral, jnp.zeros((tile - 2 * count, orders), BF16)], axis=0)
    coef = dot_t(hot_v[...], spectral).astype(BF16)
    for ty in range(2):
        base = ty * 4 * block
        coef_own[ty] = coef[base : base + block]
        for p in range(1, 4):
            coef_send[ty, p - 1] = coef[base + p * block : base + (p + 1) * block]
    for p in (2, 3, 1):
        for ty in range(2):
            coef_copy(ty, p).start()

    order_load.wait()

    def permute_step(t, carry):
        permute(t)
        return carry

    lax.fori_loop(1, AHEAD + 1, permute_step, 0)

    source = lax.broadcasted_iota(jnp.int32, (tile, cycles * tile), 0)
    target = lax.broadcasted_iota(jnp.int32, (tile, cycles * tile), 1)
    channel = 2 * ((source // cycles) % maps) + source // count
    same = (source % cycles == target // tile) & (channel == target % channels) & (source < 2 * count)
    expand = jnp.where(same, 1.0, 0.0).astype(BF16)
    depth = 4 * cycles * GROUP
    keep = lax.broadcasted_iota(jnp.int32, (depth, tile), 0) % GROUP == (
        lax.broadcasted_iota(jnp.int32, (depth, tile), 1) // channels
    )
    for ty in range(2):
        spread = []
        with jax.named_scope("waitcoef"):
            whole(coef_recv.at[ty], coef_sems.at[ty]).wait()
        for p in range(4):
            values = coef_recv[ty, p - 1] if p else coef_own[ty]
            spread.append(dot(values, expand))
        for g in range(block // GROUP):
            pieces = [
                spread[p][g * GROUP : (g + 1) * GROUP, r * tile : (r + 1) * tile]
                for p in range(4)
                for r in range(cycles)
            ]
            stacked = jnp.where(keep, jnp.concatenate(pieces, axis=0), 0.0)
            lhs_v[ty, g] = stacked.T.astype(BF16)

    high_rows = GROUP * channels

    def product(ty, t, g):
        span = slice(g * GROUP, (g + 1) * GROUP)
        parts = [own0[ty, t, :, span, :]] + [recv0[ty, t, p, :, span, :] for p in range(3)]
        right = jnp.concatenate([v.reshape(cycles * GROUP, width) for v in parts], axis=0)
        return dot(lhs_v[ty, g], right)

    def first_step(t, sent, kept):
        for ty in range(2):
            with jax.named_scope("wait0"):
                whole(recv0.at[ty, t], sems0.at[t % SLOTS, ty]).wait()
            for i, g in enumerate(sent):
                halves[0][ty, t, i * high_rows : (i + 1) * high_rows, :] = product(ty, t, g).astype(BF16)
            half_copy(0, ty, t).start()
        for ty in range(2):
            for i, g in enumerate(kept):
                acc_v[ty, t, i * high_rows : (i + 1) * high_rows, :] = product(ty, t, g)

    def next_step(s, t):
        size = rows0 >> (s + 1)
        for ty in range(2):
            with jax.named_scope(f"wait{s}"):
                half_copy(s - 1, ty, t).wait_recv()
            got = halves[2 * s - 1]
            value = acc_v[ty, t, size : 2 * size, :] + got[ty, t, size:, :].astype(F32)
            halves[2 * s][ty, t] = value.astype(BF16)
            half_copy(s, ty, t).start()
            acc_v[ty, t, :size, :] = acc_v[ty, t, :size, :] + got[ty, t, :size, :].astype(F32)

    def pow_copy(u):
        return pltpu.make_async_remote_copy(
            src_ref=pow_v.at[u],
            dst_ref=pow_recv.at[me // sharers],
            send_sem=sent_sems.at[2 + steps],
            recv_sem=pow_sem,
            device_id=at(u * sharers + me % sharers),
            device_id_type=MESH,
        )

    def last_step(t):
        size = rows0 >> steps
        ell = t * width + lax.broadcasted_iota(jnp.int32, (channels, width), 1)
        total = [None] * (maps // 2 + 1)
        lanes = pl.ds(pl.multiple_of(t * width, width), width)
        for ty in range(2):
            with jax.named_scope("waitlast"):
                half_copy(steps - 1, ty, t).wait_recv()
            value = acc_v[ty, t, :size, :] + halves[2 * steps - 1][ty, t].astype(F32)
            for i in range(per_type):
                order = owner_smem[me * own + ty * per_type + i]
                mode = jnp.where(ell >= order, value[i * channels : (i + 1) * channels], 0.0)
                row = (ty * per_type + i) * maps
                for a in range(maps):
                    harm_ref[row + a, :, lanes] = mode[2 * a : 2 * a + 2]
                heavy = mode * jnp.where(order == 0, 1.0, 2.0)
                for k in range(maps // 2 + 1):
                    turned = mode if k == 0 else jnp.concatenate([mode[2 * k :], mode[: 2 * k]], axis=0)
                    term = heavy * turned
                    total[k] = term if total[k] is None else total[k] + term
        rows = []
        for i in range(maps):
            for jj in range(i, maps):
                k, a = (jj - i, i) if jj - i <= maps // 2 else (maps - (jj - i), jj)
                rows.append(total[k][2 * a : 2 * a + 1] + total[k][2 * a + 1 : 2 * a + 2])
        power = jnp.concatenate(rows, axis=0)
        for h in range(width // tile):
            u = t * (width // tile) + h
            pow_v[u] = power[:, h * tile : (h + 1) * tile]

            @pl.when(u != me // sharers)
            def _():
                pow_copy(u).start()

    lags = [0, LAGS[0]]
    for s in range(2, steps):
        lags.append(lags[-1] + LAGS[1])
    end = lags[-1] + LAGS[2]

    def main(t, carry):
        @pl.when((t > 0) & (t + AHEAD < chunks))
        def _():
            permute(t + AHEAD)

        @pl.when(t < swap_from)
        def _():
            with jax.named_scope("first"):
                first_step(t, (2, 3), (0, 1))

        @pl.when((t >= swap_from) & (t < chunks))
        def _():
            with jax.named_scope("first"):
                first_step(t, (1, 3), (0, 2))

        for s in range(1, steps):

            @pl.when((t >= lags[s]) & (t < chunks + lags[s]))
            def _():
                with jax.named_scope(f"next{s}"):
                    next_step(s, t - lags[s])

        @pl.when(t >= end)
        def _():
            with jax.named_scope("last"):
                last_step(t - end)

        return carry

    lax.fori_loop(0, chunks + end, main, 0)

    mine = me // sharers
    total = pow_v[mine]
    with scope("waitpow"):
        whole(pow_recv.at[: tiles - 1], pow_sem).wait()
    for u in range(tiles):
        total = total + jnp.where(u != mine, pow_recv[u], 0.0)
    pow_mine[...] = total

    def pair_copy(e):
        return pltpu.make_async_remote_copy(
            src_ref=pow_mine,
            dst_ref=pow_pair.at[e - 1],
            send_sem=pair_sems.at[0, e - 1],
            recv_sem=pair_sems.at[1, e - 1],
            device_id=at(mine * sharers + (me + e) % sharers),
            device_id_type=MESH,
        )

    for e in range(1, sharers):
        pair_copy(e).start()
    for e in range(1, sharers):
        with jax.named_scope("waitpair"):
            pair_copy(e).wait_recv()
        total = total + pow_pair[e - 1]
    ell = mine * tile + lax.broadcasted_iota(jnp.int32, total.shape, 1)
    total = total / (2 * ell + 1).astype(F32)
    share = tile // sharers
    turned = total
    for c in range(1, sharers):
        shifted = jnp.concatenate([total[:, c * share :], total[:, : c * share]], axis=1)
        turned = jnp.where(me % sharers == c, shifted, turned)
    spec_ref[...] = turned[:, :share]

    with jax.named_scope("drain"):
        whole(send0, sent_sems.at[0]).wait()
        whole(coef_send, sent_sems.at[1]).wait()
        for s in range(steps):
            whole(halves[2 * s], sent_sems.at[2 + s]).wait()
    for e in range(1, sharers):
        pair_copy(e).wait_send()
    whole(pow_v.at[: tiles - 1], sent_sems.at[2 + steps]).wait()


def hand_over_body(large_ref, small_ref, large_out, small_out, sems):
    copies = [
        pltpu.make_async_copy(large_ref, large_out, sems.at[0]),
        pltpu.make_async_copy(small_ref, small_out, sems.at[1]),
    ]
    for copy in copies:
        copy.start()
    for copy in copies:
        copy.wait()


def hand_over(large, small):
    return pl.pallas_call(
        hand_over_body,
        out_shape=[jax.ShapeDtypeStruct(large.shape, large.dtype), jax.ShapeDtypeStruct(small.shape, small.dtype)],
        in_specs=[pl.BlockSpec(memory_space=pltpu.VMEM)] * 2,
        out_specs=[pl.BlockSpec(memory_space=pl.ANY)] * 2,
        scratch_shapes=[pltpu.SemaphoreType.DMA((2,))],
        cost_estimate=pl.CostEstimate(flops=large.size, bytes_accessed=8 * large.size, transcendentals=0),
    )(large, small)


def per_device(sky_maps, legendre, owner_table):
    maps, cycles, pixels = sky_maps.shape
    _, orders, ells = legendre.shape
    devices = lax.axis_size(AXES)
    grp = lax.axis_size(AXES[1])
    bits = devices.bit_length() - 1
    steps = bits - 2
    width = WIDTH
    chunks = ells // width
    channels = 2 * maps
    own = orders // devices
    block = orders // 8
    tile = 128
    coarse = pixels // tile
    tiles = ells // tile
    sharers = tile * devices // ells
    pairs = maps * (maps + 1) // 2
    first, high, low = fourier_tables(pixels, orders, tile)
    rows0 = block * channels
    halves = []
    for s in range(steps):
        halves += [pltpu.VMEM((2, chunks, rows0 >> (s + 1), width), BF16)] * 2
    cfg = (maps, cycles, orders, ells, devices, grp, width)
    scratch = [
        pltpu.SMEM((orders,), jnp.int32),
        pltpu.VMEM((1, orders), jnp.int32),
        pltpu.VMEM((chunks, cycles, orders, width), BF16),
        pltpu.VMEM((maps, cycles, coarse, tile), F32),
        pltpu.VMEM(first.shape, F32),
        pltpu.VMEM(high.shape, BF16),
        pltpu.VMEM(low.shape, BF16),
        pltpu.VMEM((orders, orders), BF16),
        pltpu.VMEM((2, block // GROUP, GROUP * channels, 4 * cycles * GROUP), BF16),
        pltpu.VMEM((2, chunks, cycles, block, width), BF16),
        pltpu.VMEM((2, chunks, 3, cycles, block, width), BF16),
        pltpu.VMEM((2, chunks, 3, cycles, block, width), BF16),
        pltpu.VMEM((2, block, tile), BF16),
        pltpu.VMEM((2, 3, block, tile), BF16),
        pltpu.VMEM((2, 3, block, tile), BF16),
        pltpu.VMEM((2, chunks, rows0 // 2, width), F32),
        halves,
        pltpu.VMEM((tiles, pairs, tile), F32),
        pltpu.VMEM((tiles, pairs, tile), F32),
        pltpu.VMEM((pairs, tile), F32),
        pltpu.VMEM((sharers - 1, pairs, tile), F32),
        pltpu.SemaphoreType.DMA((4,)),
        pltpu.SemaphoreType.DMA,
        pltpu.SemaphoreType.DMA((5,)),
        pltpu.SemaphoreType.DMA((3 + steps,)),
        pltpu.SemaphoreType.DMA((SLOTS, 2)),
        pltpu.SemaphoreType.DMA((2,)),
        pltpu.SemaphoreType.DMA((steps, SLOTS, 2)),
        pltpu.SemaphoreType.DMA,
        pltpu.SemaphoreType.DMA((2, sharers - 1)),
    ]
    anywhere = pl.BlockSpec(memory_space=pl.ANY)
    vmem = pl.BlockSpec(memory_space=pltpu.VMEM)
    harmonics, spectra = pl.pallas_call(
        functools.partial(kernel, cfg),
        out_shape=[
            pltpu.VMEM((own * maps, 2, ells), F32),
            pltpu.VMEM((pairs, ells // devices), F32),
        ],
        in_specs=[anywhere] * 7,
        out_specs=[vmem, vmem],
        scratch_shapes=scratch,
        compiler_params=pltpu.CompilerParams(
            vmem_limit_bytes=56 * MIB, collective_id=0, has_side_effects=True
        ),
        cost_estimate=pl.CostEstimate(
            flops=2 * cycles * orders * orders * ells, bytes_accessed=2 * legendre.size, transcendentals=0
        ),
    )(
        owner_table,
        owner_table.reshape(1, orders),
        sky_maps,
        jnp.asarray(first),
        jnp.asarray(high),
        jnp.asarray(low),
        legendre,
    )
    harmonics, spectra = (pltpu.with_memory_space_constraint(v, pltpu.VMEM) for v in (harmonics, spectra))
    harmonics, spectra = hand_over(harmonics, spectra)
    return harmonics.reshape(own, maps, 2, ells), spectra


def solution(mesh):
    return jax.shard_map(
        per_device,
        mesh=mesh,
        in_specs=(P(None, AXES, None), P(AXES, None, None), P()),
        out_specs=(P(AXES, None, None, None), P(None, AXES)),
        check_vma=False,
    )
```

```python
import functools
import math

import jax
import jax.numpy as jnp
import numpy as np
from jax import lax
from jax.experimental import pallas as pl
from jax.experimental.pallas import tpu as pltpu
from jax.sharding import PartitionSpec as P

AXES = ("blk", "grp")
MIB = 1024 * 1024
MESH = pl.DeviceIdType.MESH
BF16 = jnp.bfloat16
F32 = jnp.float32
GROUP = 16
FIRST = (1, 2)
EARLY = 3
WIDTH = 128
AHEAD = 3
CROSS = 1
SWAPPED = 2
SLOTS = 8
LAGS = (2, 2, 3)


def plan_of(bits):
    later = [[EARLY] + [b for b in range(1, bits) if b not in (first, EARLY)] for first in FIRST]
    return later


def flip(me, bits):
    out = me
    for b in bits:
        out = out + (1 - 2 * ((me // (1 << b)) % 2)) * (1 << b)
    return out


def split_bf16(values):
    high = values.astype(BF16)
    low = (values - high.astype(F32)).astype(BF16)
    return high, low


def dot(left, right):
    return jnp.dot(left, right, preferred_element_type=F32)


def dot_t(left, right):
    return lax.dot_general(left, right, (((1,), (1,)), ((), ())), preferred_element_type=F32)


def fourier_tables(pixels, order_count, width):
    coarse = pixels // width
    k1, m1 = np.meshgrid(np.arange(coarse), np.arange(coarse), indexing="ij")
    angle = 2.0 * math.pi * ((k1 * m1) % coarse) / coarse
    first = np.concatenate([np.cos(angle.T), -np.sin(angle.T)], axis=0)
    k2 = np.arange(width)[:, None]
    m = np.arange(order_count)[None, :]
    angle = 2.0 * math.pi * ((k2 * m) % pixels) / pixels
    cosine, sine = np.cos(angle) / math.sqrt(pixels), np.sin(angle) / math.sqrt(pixels)
    second = np.block([[cosine, -sine], [sine, cosine]]).astype(np.float32)
    high = second.astype(jnp.bfloat16)
    low = (second - high.astype(np.float32)).astype(jnp.bfloat16)
    return first.astype(np.float32), high, low


def kernel(
    cfg, owner_hbm, owner_row_hbm, sky_hbm, first_hbm, high_hbm, low_hbm, leg_hbm, harm_ref, spec_ref,
    owner_smem, owner_ref, leg_v, sky_v, first_v, high_v, low_v, hot_v, lhs_v, own0, send0, recv0, coef_own, coef_send, coef_recv,
    acc_v, halves, pow_v, pow_recv, pow_mine, pow_pair, load_sem, sky_sem, table_sem,
    sent_sems, sems0, coef_sems, half_sems, pow_sem, pair_sems,
):
    maps, cycles, orders, ells, devices, grp, width = cfg
    bits = devices.bit_length() - 1
    later = plan_of(bits)
    steps = bits - 2
    chunks = ells // width
    channels = 2 * maps
    own = orders // devices
    per_type = own // 2
    block = orders // 8
    rows0 = block * channels
    me = lax.axis_index("blk") * grp + lax.axis_index("grp")
    tile = 128
    tiles = ells // tile
    sharers = tile * devices // ells
    pairs = maps * (maps + 1) // 2

    def at(index):
        return (index // grp, index % grp)

    def bit(b):
        return (me // (1 << b)) % 2

    gather = [
        [[None, flip(me, [0]), flip(me, [b]), flip(me, [b, 0])] for b in firsts] for firsts in (FIRST, (EARLY, EARLY))
    ]
    near = sorted({(b,) for b in range(bits)} | {(0, b) for b in FIRST + (EARLY,)})

    def group_row(variant, p, g):
        q = p * 4 + g if variant == 0 else (g // 2) * 8 + (p % 2) * 4 + (p // 2) * 2 + g % 2
        return q * GROUP

    scope = jax.named_scope
    row_load = pltpu.make_async_copy(owner_row_hbm, owner_ref, table_sem.at[3])
    row_load.start()
    barrier = pltpu.get_barrier_semaphore()
    for masks in near:
        pl.semaphore_signal(barrier, inc=1, device_id=at(flip(me, masks)), device_id_type=MESH)

    def load(t):
        lanes = pl.ds(pl.multiple_of(t * width, width), width)
        return pltpu.make_async_copy(leg_hbm.at[:, :, lanes], leg_v.at[t], load_sem.at[t % 4])

    def load_start(t, carry):
        load(t).start()
        return carry

    with scope("startload"):
        lax.fori_loop(0, 4, load_start, 0)
    coarse = sky_v.shape[2]

    def sky_load(k):
        lanes = pl.ds(k * tile, tile)
        return pltpu.make_async_copy(sky_hbm.at[:, :, lanes], sky_v.at[:, :, k, :], sky_sem)

    for k in range(coarse):
        sky_load(k).start()
    tables = [
        pltpu.make_async_copy(src, dst, table_sem.at[i])
        for i, (src, dst) in enumerate(((first_hbm, first_v), (high_hbm, high_v), (low_hbm, low_v)))
    ]
    for table in tables:
        table.start()


    j = lax.broadcasted_iota(jnp.int32, (orders, tile), 0)
    half_bit, block_bit = (orders // 2).bit_length() - 1, block.bit_length() - 1
    part = j >> half_bit
    slot = part * per_type + (j & (per_type - 1))

    def place(b, differs):
        mine = bit(b)
        return (mine + differs - 2 * mine * differs) * ((1 << b) * own)

    slot = slot + place(0, (j >> block_bit) & 1)
    for ty in range(2):
        terms = place(FIRST[ty], (j >> (block_bit + 1)) & 1)
        for s, b in enumerate(later[ty]):
            terms = terms + place(b, (j >> (block_bit - s - 1)) & 1)
        slot = slot + jnp.where(part == ty, terms, 0)
    lane = lax.broadcasted_iota(jnp.int32, (orders, tile), 1)
    pick = jnp.concatenate(
        [jnp.where(slot == lane + c * tile, 1.0, 0.0).astype(BF16) for c in range(orders // tile)], axis=1
    )
    row_load.wait()
    table = jnp.where(lax.broadcasted_iota(jnp.int32, (orders, orders), 0) == owner_ref[...], 1.0, 0.0).astype(BF16)
    hot_v[...] = dot_t(pick, table).astype(BF16)

    def whole(ref, sem):
        return pltpu.make_async_copy(ref, ref, sem)

    def gather_copy(ty, t, p, variant):
        return pltpu.make_async_remote_copy(
            src_ref=send0.at[ty, t, p - 1],
            dst_ref=recv0.at[ty, t, p - 1],
            send_sem=sent_sems.at[0],
            recv_sem=sems0.at[t % SLOTS, ty],
            device_id=at(gather[variant][ty][p]),
            device_id_type=MESH,
        )

    def coef_copy(variant, ty, p):
        return pltpu.make_async_remote_copy(
            src_ref=coef_send.at[variant, ty, p - 1],
            dst_ref=coef_recv.at[variant, ty, p - 1],
            send_sem=sent_sems.at[1],
            recv_sem=coef_sems.at[variant, ty],
            device_id=at(gather[variant][ty][p]),
            device_id_type=MESH,
        )

    swap_from = chunks - SWAPPED
    groups = block // GROUP

    def half_copy(s, ty, t):
        partner = flip(me, [later[ty][s]])
        if s < 2:
            partner = jnp.where(t < swap_from, partner, flip(me, [later[ty][1 - s]]))
        if s == 0:
            partner = jnp.where(t == CROSS, flip(me, [FIRST[ty]]), partner)
        return pltpu.make_async_remote_copy(
            src_ref=halves[2 * s].at[ty, t],
            dst_ref=halves[2 * s + 1].at[ty, t],
            send_sem=sent_sems.at[2 + s],
            recv_sem=half_sems.at[s, t % SLOTS, ty],
            device_id=at(partner),
            device_id_type=MESH,
        )

    def permute(t, variant=0):
        with jax.named_scope("load"):
            load(t).wait()
        with jax.named_scope("permute"):
            permute_loaded(t, variant)

        @pl.when(t + 4 < chunks)
        def _():
            load(t + 4).start()

    def permute_loaded(t, variant):
        together = max(1, 256 // width)
        for r0 in range(0, cycles, together):
            values = jnp.concatenate([leg_v[t, r0 + i] for i in range(together)], axis=1)
            for ty in range(2):
                picked = dot(hot_v[ty * 4 * block : (ty + 1) * 4 * block, :], values).astype(BF16)
                for i in range(together):
                    piece = picked[:, i * width : (i + 1) * width]
                    for p in range(4):
                        rows = [group_row(variant, p, g) for g in range(groups)]
                        rows = jnp.concatenate([piece[row : row + GROUP] for row in rows], axis=0)
                        if p == 0:
                            own0[ty, t, r0 + i] = rows
                        else:
                            send0[ty, t, p - 1, r0 + i] = rows
        for p in (2, 3, 1):
            for ty in range(2):
                gather_copy(ty, t, p, variant).start()

    with jax.named_scope("barrier"):
        pl.semaphore_wait(barrier, len(near))
    permute(0)
    permute(CROSS, 1)
    order_load = pltpu.make_async_copy(owner_hbm, owner_smem, table_sem.at[4])
    order_load.start()

    with jax.named_scope("waitsky"):
        whole(sky_v, sky_sem).wait()
    for table in tables:
        table.wait()
    count = maps * cycles
    columns = 2 * orders
    stages = []
    first = first_v[...]
    for b in range(count):
        stage = jnp.dot(
            first, sky_v[b // cycles, b % cycles], precision=lax.Precision.HIGHEST, preferred_element_type=F32
        )
        stages.append(jnp.concatenate([stage[:coarse], stage[coarse:]], axis=1))
    left_high, left_low = split_bf16(jnp.concatenate(stages, axis=0))
    spectral = []
    span = orders // 2
    for c in range(columns // span):
        picked = slice(c * span, (c + 1) * span)
        full = dot(left_high, high_v[:, picked]) + (dot(left_high, low_v[:, picked]) + dot(left_low, high_v[:, picked]))
        full = full.reshape(count, coarse, span)
        m1 = lax.broadcasted_iota(jnp.int32, (1, coarse, span), 1)
        col = lax.broadcasted_iota(jnp.int32, (1, coarse, span), 2)
        spectral.append(jnp.sum(jnp.where(col % coarse == m1, full, 0.0), axis=1))
    spectral = jnp.concatenate(
        [jnp.concatenate(spectral[:2], axis=1), jnp.concatenate(spectral[2:], axis=1)], axis=0
    ).astype(BF16)
    copies = tile // (2 * count)
    coef = dot_t(hot_v[...], jnp.concatenate([spectral] * copies, axis=0))
    lane_group = lax.broadcasted_iota(jnp.int32, (GROUP, tile), 1) // (2 * count)
    for variant in range(2):
        for ty in range(2):
            for p in range(4):
                packed = None
                for g in range(groups):
                    row = ty * 4 * block + group_row(variant, p, g)
                    rows = coef[row : row + GROUP]
                    packed = rows if packed is None else jnp.where(lane_group == g, rows, packed)
                if p == 0:
                    coef_own[variant, ty] = packed.astype(BF16)
                else:
                    coef_send[variant, ty, p - 1] = packed.astype(BF16)
    for variant in range(2):
        for p in (2, 3, 1):
            for ty in range(2):
                coef_copy(variant, ty, p).start()

    order_load.wait()

    def permute_step(t, carry):
        permute(t)
        return carry

    lax.fori_loop(CROSS + 1, AHEAD + 1, permute_step, 0)

    source = lax.broadcasted_iota(jnp.int32, (tile, cycles * tile), 0)
    target = lax.broadcasted_iota(jnp.int32, (tile, cycles * tile), 1)
    channel = 2 * ((source // cycles) % maps) + (source // count) % 2
    same = (source % cycles == target // tile) & (channel == target % channels)
    expand = jnp.where(same, 1.0, 0.0).astype(BF16)
    depth = 4 * cycles * GROUP
    keep = lax.broadcasted_iota(jnp.int32, (depth, tile), 0) % GROUP == (
        lax.broadcasted_iota(jnp.int32, (depth, tile), 1) // channels
    )
    pack_group = lax.broadcasted_iota(jnp.int32, (4 * GROUP, tile), 1) // (2 * count)

    def build(variant):
        for ty in range(2):
            with scope("waitcoef"):
                whole(coef_recv.at[variant, ty], coef_sems.at[variant, ty]).wait()
            values = [coef_own[variant, ty]] + [coef_recv[variant, ty, p] for p in range(3)]
            values = jnp.concatenate(values, axis=0).astype(F32)
            for g in range(groups):
                spread = dot(jnp.where(pack_group == g, values, 0.0).astype(BF16), expand)
                pieces = [
                    spread[p * GROUP : (p + 1) * GROUP, r * tile : (r + 1) * tile]
                    for p in range(4)
                    for r in range(cycles)
                ]
                stacked = jnp.where(keep, jnp.concatenate(pieces, axis=0), 0.0)
                lhs_v[variant, ty, g] = stacked.T.astype(BF16)

    build(0)
    high_rows = GROUP * channels

    def product(variant, ty, t, g):
        span = slice(g * GROUP, (g + 1) * GROUP)
        parts = [own0[ty, t, :, span, :]] + [recv0[ty, t, p, :, span, :] for p in range(3)]
        right = jnp.concatenate([v.reshape(cycles * GROUP, width) for v in parts], axis=0)
        return dot(lhs_v[variant, ty, g], right)

    def first_step(t, sent, kept, variant=0):
        for ty in range(2):
            with jax.named_scope("wait0"):
                whole(recv0.at[ty, t], sems0.at[t % SLOTS, ty]).wait()
            for i, g in enumerate(sent):
                halves[0][ty, t, i * high_rows : (i + 1) * high_rows, :] = product(variant, ty, t, g).astype(BF16)
            half_copy(0, ty, t).start()
        for ty in range(2):
            for i, g in enumerate(kept):
                acc_v[ty, t, i * high_rows : (i + 1) * high_rows, :] = product(variant, ty, t, g)

    def next_step(s, t):
        size = rows0 >> (s + 1)
        for ty in range(2):
            with jax.named_scope(f"wait{s}"):
                half_copy(s - 1, ty, t).wait_recv()
            got = halves[2 * s - 1]
            value = acc_v[ty, t, size : 2 * size, :] + got[ty, t, size:, :].astype(F32)
            halves[2 * s][ty, t] = value.astype(BF16)
            half_copy(s, ty, t).start()
            acc_v[ty, t, :size, :] = acc_v[ty, t, :size, :] + got[ty, t, :size, :].astype(F32)

    def pow_copy(u):
        return pltpu.make_async_remote_copy(
            src_ref=pow_v.at[u],
            dst_ref=pow_recv.at[me // sharers],
            send_sem=sent_sems.at[2 + steps],
            recv_sem=pow_sem,
            device_id=at(u * sharers + me % sharers),
            device_id_type=MESH,
        )

    def last_step(t):
        size = rows0 >> steps
        ell = t * width + lax.broadcasted_iota(jnp.int32, (channels, width), 1)
        total = [None] * (maps // 2 + 1)
        lanes = pl.ds(pl.multiple_of(t * width, width), width)
        for ty in range(2):
            with jax.named_scope("waitlast"):
                half_copy(steps - 1, ty, t).wait_recv()
            value = acc_v[ty, t, :size, :] + halves[2 * steps - 1][ty, t].astype(F32)
            for i in range(per_type):
                order = owner_smem[me * own + ty * per_type + i]
                mode = jnp.where(ell >= order, value[i * channels : (i + 1) * channels], 0.0)
                row = (ty * per_type + i) * maps
                for a in range(maps):
                    harm_ref[row + a, :, lanes] = mode[2 * a : 2 * a + 2]
                heavy = mode * jnp.where(order == 0, 1.0, 2.0)
                for k in range(maps // 2 + 1):
                    turned = mode if k == 0 else jnp.concatenate([mode[2 * k :], mode[: 2 * k]], axis=0)
                    term = heavy * turned
                    total[k] = term if total[k] is None else total[k] + term
        rows = []
        for i in range(maps):
            for jj in range(i, maps):
                k, a = (jj - i, i) if jj - i <= maps // 2 else (maps - (jj - i), jj)
                rows.append(total[k][2 * a : 2 * a + 1] + total[k][2 * a + 1 : 2 * a + 2])
        power = jnp.concatenate(rows, axis=0)
        for h in range(width // tile):
            u = t * (width // tile) + h
            pow_v[u] = power[:, h * tile : (h + 1) * tile]

            @pl.when(u != me // sharers)
            def _():
                pow_copy(u).start()

    lags = [0, LAGS[0]]
    for s in range(2, steps):
        lags.append(lags[-1] + LAGS[1])
    end = lags[-1] + LAGS[2]

    def main(t, carry):
        @pl.when((t > 0) & (t + AHEAD < chunks))
        def _():
            permute(t + AHEAD)

        @pl.when((t < swap_from) & (t != CROSS))
        def _():
            with jax.named_scope("first"):
                first_step(t, (2, 3), (0, 1))

        @pl.when(t == CROSS)
        def _():
            with jax.named_scope("build"):
                build(1)
            with jax.named_scope("first"):
                first_step(t, (2, 3), (0, 1), 1)

        @pl.when((t >= swap_from) & (t < chunks))
        def _():
            with jax.named_scope("first"):
                first_step(t, (1, 3), (0, 2))

        for s in range(1, steps):

            @pl.when((t >= lags[s]) & (t < chunks + lags[s]))
            def _():
                with jax.named_scope(f"next{s}"):
                    next_step(s, t - lags[s])

        @pl.when(t >= end)
        def _():
            with jax.named_scope("last"):
                last_step(t - end)

        return carry

    lax.fori_loop(0, chunks + end, main, 0)

    mine = me // sharers
    total = pow_v[mine]
    with scope("waitpow"):
        whole(pow_recv.at[: tiles - 1], pow_sem).wait()
    for u in range(tiles):
        total = total + jnp.where(u != mine, pow_recv[u], 0.0)
    pow_mine[...] = total

    def pair_copy(e):
        return pltpu.make_async_remote_copy(
            src_ref=pow_mine,
            dst_ref=pow_pair.at[e - 1],
            send_sem=pair_sems.at[0, e - 1],
            recv_sem=pair_sems.at[1, e - 1],
            device_id=at(mine * sharers + (me + e) % sharers),
            device_id_type=MESH,
        )

    for e in range(1, sharers):
        pair_copy(e).start()
    for e in range(1, sharers):
        with jax.named_scope("waitpair"):
            pair_copy(e).wait_recv()
        total = total + pow_pair[e - 1]
    ell = mine * tile + lax.broadcasted_iota(jnp.int32, total.shape, 1)
    total = total / (2 * ell + 1).astype(F32)
    share = tile // sharers
    turned = total
    for c in range(1, sharers):
        shifted = jnp.concatenate([total[:, c * share :], total[:, : c * share]], axis=1)
        turned = jnp.where(me % sharers == c, shifted, turned)
    spec_ref[...] = turned[:, :share]

    with jax.named_scope("drain"):
        whole(send0, sent_sems.at[0]).wait()
        whole(coef_send, sent_sems.at[1]).wait()
        for s in range(steps):
            whole(halves[2 * s], sent_sems.at[2 + s]).wait()
    for e in range(1, sharers):
        pair_copy(e).wait_send()
    whole(pow_v.at[: tiles - 1], sent_sems.at[2 + steps]).wait()


def hand_over_body(large_ref, small_ref, large_out, small_out, sems):
    copies = [
        pltpu.make_async_copy(large_ref, large_out, sems.at[0]),
        pltpu.make_async_copy(small_ref, small_out, sems.at[1]),
    ]
    for copy in copies:
        copy.start()
    for copy in copies:
        copy.wait()


def hand_over(large, small):
    return pl.pallas_call(
        hand_over_body,
        out_shape=[jax.ShapeDtypeStruct(large.shape, large.dtype), jax.ShapeDtypeStruct(small.shape, small.dtype)],
        in_specs=[pl.BlockSpec(memory_space=pltpu.VMEM)] * 2,
        out_specs=[pl.BlockSpec(memory_space=pl.ANY)] * 2,
        scratch_shapes=[pltpu.SemaphoreType.DMA((2,))],
        cost_estimate=pl.CostEstimate(flops=large.size, bytes_accessed=8 * large.size, transcendentals=0),
    )(large, small)


def per_device(sky_maps, legendre, owner_table):
    maps, cycles, pixels = sky_maps.shape
    _, orders, ells = legendre.shape
    devices = lax.axis_size(AXES)
    grp = lax.axis_size(AXES[1])
    bits = devices.bit_length() - 1
    steps = bits - 2
    width = WIDTH
    chunks = ells // width
    channels = 2 * maps
    own = orders // devices
    block = orders // 8
    tile = 128
    coarse = pixels // tile
    tiles = ells // tile
    sharers = tile * devices // ells
    pairs = maps * (maps + 1) // 2
    first, high, low = fourier_tables(pixels, orders, tile)
    rows0 = block * channels
    halves = []
    for s in range(steps):
        halves += [pltpu.VMEM((2, chunks, rows0 >> (s + 1), width), BF16)] * 2
    cfg = (maps, cycles, orders, ells, devices, grp, width)
    scratch = [
        pltpu.SMEM((orders,), jnp.int32),
        pltpu.VMEM((1, orders), jnp.int32),
        pltpu.VMEM((chunks, cycles, orders, width), BF16),
        pltpu.VMEM((maps, cycles, coarse, tile), F32),
        pltpu.VMEM(first.shape, F32),
        pltpu.VMEM(high.shape, BF16),
        pltpu.VMEM(low.shape, BF16),
        pltpu.VMEM((orders, orders), BF16),
        pltpu.VMEM((2, 2, block // GROUP, GROUP * channels, 4 * cycles * GROUP), BF16),
        pltpu.VMEM((2, chunks, cycles, block, width), BF16),
        pltpu.VMEM((2, chunks, 3, cycles, block, width), BF16),
        pltpu.VMEM((2, chunks, 3, cycles, block, width), BF16),
        pltpu.VMEM((2, 2, GROUP, tile), BF16),
        pltpu.VMEM((2, 2, 3, GROUP, tile), BF16),
        pltpu.VMEM((2, 2, 3, GROUP, tile), BF16),
        pltpu.VMEM((2, chunks, rows0 // 2, width), F32),
        halves,
        pltpu.VMEM((tiles, pairs, tile), F32),
        pltpu.VMEM((tiles, pairs, tile), F32),
        pltpu.VMEM((pairs, tile), F32),
        pltpu.VMEM((sharers - 1, pairs, tile), F32),
        pltpu.SemaphoreType.DMA((4,)),
        pltpu.SemaphoreType.DMA,
        pltpu.SemaphoreType.DMA((5,)),
        pltpu.SemaphoreType.DMA((3 + steps,)),
        pltpu.SemaphoreType.DMA((SLOTS, 2)),
        pltpu.SemaphoreType.DMA((2, 2)),
        pltpu.SemaphoreType.DMA((steps, SLOTS, 2)),
        pltpu.SemaphoreType.DMA,
        pltpu.SemaphoreType.DMA((2, sharers - 1)),
    ]
    anywhere = pl.BlockSpec(memory_space=pl.ANY)
    vmem = pl.BlockSpec(memory_space=pltpu.VMEM)
    harmonics, spectra = pl.pallas_call(
        functools.partial(kernel, cfg),
        out_shape=[
            pltpu.VMEM((own * maps, 2, ells), F32),
            pltpu.VMEM((pairs, ells // devices), F32),
        ],
        in_specs=[anywhere] * 7,
        out_specs=[vmem, vmem],
        scratch_shapes=scratch,
        compiler_params=pltpu.CompilerParams(
            vmem_limit_bytes=56 * MIB, collective_id=0, has_side_effects=True
        ),
        cost_estimate=pl.CostEstimate(
            flops=2 * cycles * orders * orders * ells, bytes_accessed=2 * legendre.size, transcendentals=0
        ),
    )(
        owner_table,
        owner_table.reshape(1, orders),
        sky_maps,
        jnp.asarray(first),
        jnp.asarray(high),
        jnp.asarray(low),
        legendre,
    )
    harmonics, spectra = (pltpu.with_memory_space_constraint(v, pltpu.VMEM) for v in (harmonics, spectra))
    harmonics, spectra = hand_over(harmonics, spectra)
    return harmonics.reshape(own, maps, 2, ells), spectra


def solution(mesh):
    return jax.shard_map(
        per_device,
        mesh=mesh,
        in_specs=(P(None, AXES, None), P(AXES, None, None), P()),
        out_specs=(P(AXES, None, None, None), P(None, AXES)),
        check_vma=False,
    )
```

```python
import functools
import math

import jax
import jax.numpy as jnp
import numpy as np
from jax import lax
from jax.experimental import pallas as pl
from jax.experimental.pallas import tpu as pltpu
from jax.sharding import PartitionSpec as P

AXES = ("blk", "grp")
MIB = 1024 * 1024
MESH = pl.DeviceIdType.MESH
BF16 = jnp.bfloat16
F32 = jnp.float32
GROUP = 16
FIRST = (1, 2)
EARLY = 3
WIDTH = 128
AHEAD = 3
CROSS = 1
SWAPPED = 1
FINALE = (
    *((1, 4), (0, 2), (3, 9), (3, 8), (1, 3), (0, 1), (2, 6), (2, 5), (3, 7), (2, 4), (2, 3)),
    *((1, 2), (1, 1), (3, 6), (2, 2), (3, 5), (2, 1), (3, 4), (3, 3), (3, 2), (3, 1)),
)
ROTATE = 0
SLOTS = 8
LAGS = (2, 2, 3)


def plan_of(bits):
    later = [[EARLY] + [b for b in range(1, bits) if b not in (first, EARLY)] for first in FIRST]
    return later


def flip(me, bits):
    out = me
    for b in bits:
        out = out + (1 - 2 * ((me // (1 << b)) % 2)) * (1 << b)
    return out


def split_bf16(values):
    high = values.astype(BF16)
    low = (values - high.astype(F32)).astype(BF16)
    return high, low


def dot(left, right):
    return jnp.dot(left, right, preferred_element_type=F32)


def dot_t(left, right):
    return lax.dot_general(left, right, (((1,), (1,)), ((), ())), preferred_element_type=F32)


def fourier_tables(pixels, order_count, width):
    coarse = pixels // width
    k1, m1 = np.meshgrid(np.arange(coarse), np.arange(coarse), indexing="ij")
    angle = 2.0 * math.pi * ((k1 * m1) % coarse) / coarse
    first = np.concatenate([np.cos(angle.T), -np.sin(angle.T)], axis=0)
    k2 = np.arange(width)[:, None]
    m = np.arange(order_count)[None, :]
    angle = 2.0 * math.pi * ((k2 * m) % pixels) / pixels
    cosine, sine = np.cos(angle) / math.sqrt(pixels), np.sin(angle) / math.sqrt(pixels)
    second = np.block([[cosine, -sine], [sine, cosine]]).astype(np.float32)
    high = second.astype(jnp.bfloat16)
    low = (second - high.astype(np.float32)).astype(jnp.bfloat16)
    return first.astype(np.float32), high, low


def kernel(
    cfg, owner_hbm, owner_row_hbm, sky_hbm, first_hbm, high_hbm, low_hbm, leg_hbm, harm_ref, spec_ref,
    owner_smem, owner_ref, column_v, leg_v, sky_v, first_v, high_v, low_v, hot_v, lhs_v, own0, send0, recv0, coef_own, coef_send, coef_recv,
    acc_v, halves, pow_v, pow_recv, pow_mine, pow_pair, load_sem, sky_sem, table_sem,
    sent_sems, sems0, coef_sems, half_sems, pow_sem, pair_sems,
):
    maps, cycles, orders, ells, devices, grp, width = cfg
    bits = devices.bit_length() - 1
    later = plan_of(bits)
    steps = bits - 2
    chunks = ells // width
    channels = 2 * maps
    own = orders // devices
    per_type = own // 2
    block = orders // 8
    rows0 = block * channels
    me = lax.axis_index("blk") * grp + lax.axis_index("grp")
    tile = 128
    tiles = ells // tile
    sharers = tile * devices // ells
    pairs = maps * (maps + 1) // 2

    def at(index):
        return (index // grp, index % grp)

    def bit(b):
        return (me // (1 << b)) % 2

    gather = [
        [[None, flip(me, [0]), flip(me, [b]), flip(me, [b, 0])] for b in firsts] for firsts in (FIRST, (EARLY, EARLY))
    ]
    near = sorted({(b,) for b in range(bits)} | {(0, b) for b in FIRST + (EARLY,)}, reverse=True)

    def group_row(variant, p, g):
        q = p * 4 + g if variant == 0 else (g // 2) * 8 + (p % 2) * 4 + (p // 2) * 2 + g % 2
        return q * GROUP

    scope = jax.named_scope
    row_load = pltpu.make_async_copy(owner_row_hbm, owner_ref, table_sem.at[3])
    row_load.start()
    barrier = pltpu.get_barrier_semaphore()
    for masks in near:
        pl.semaphore_signal(barrier, inc=1, device_id=at(flip(me, masks)), device_id_type=MESH)

    def place_of(t):
        return (t + ROTATE * chunks // 16) % chunks

    def load(t):
        lanes = pl.ds(pl.multiple_of(place_of(t) * width, width), width)
        return pltpu.make_async_copy(leg_hbm.at[:, :, lanes], leg_v.at[t], load_sem.at[t % 4])

    def load_start(t, carry):
        load(t).start()
        return carry

    with scope("startload"):
        lax.fori_loop(0, 4, load_start, 0)
    coarse = sky_v.shape[2]

    def sky_load(k):
        lanes = pl.ds(k * tile, tile)
        return pltpu.make_async_copy(sky_hbm.at[:, :, lanes], sky_v.at[:, :, k, :], sky_sem)

    for k in range(coarse):
        sky_load(k).start()
    tables = [
        pltpu.make_async_copy(src, dst, table_sem.at[i])
        for i, (src, dst) in enumerate(((first_hbm, first_v), (high_hbm, high_v), (low_hbm, low_v)))
    ]
    for table in tables:
        table.start()


    half_bit, block_bit = (orders // 2).bit_length() - 1, block.bit_length() - 1

    def place(b, differs):
        mine = bit(b)
        return (mine + differs - 2 * mine * differs) * ((1 << b) * own)

    lane = lax.broadcasted_iota(jnp.int32, (orders, tile), 1)
    if per_type % 8 == 0:
        places = [[place(b, differs) for differs in range(2)] for b in range(bits)]
        row_load.wait()
        for c in range(orders // tile):
            row = owner_ref[:, c * tile : (c + 1) * tile].astype(F32)
            column_v[c * tile : (c + 1) * tile, :] = jnp.broadcast_to(row, (tile, tile)).T
        picked = []
        for jb in range(0, orders, 8):
            ty = jb >> half_bit
            start = ty * per_type + jb % per_type + places[0][(jb >> block_bit) & 1]
            start = start + places[FIRST[ty]][(jb >> (block_bit + 1)) & 1]
            for s, b in enumerate(later[ty]):
                start = start + places[b][(jb >> (block_bit - s - 1)) & 1]
            picked.append(column_v[pl.ds(pl.multiple_of(start, 8), 8), :])
        column = jnp.concatenate(picked, axis=0)
        lane = lane.astype(F32)
        for c in range(orders // tile):
            hot_v[:, c * tile : (c + 1) * tile] = jnp.where(column == lane + float(c * tile), 1.0, 0.0).astype(BF16)
    else:
        j = lax.broadcasted_iota(jnp.int32, (orders, tile), 0)
        part = j >> half_bit
        slot = part * per_type + (j & (per_type - 1)) + place(0, (j >> block_bit) & 1)
        for ty in range(2):
            terms = place(FIRST[ty], (j >> (block_bit + 1)) & 1)
            for s, b in enumerate(later[ty]):
                terms = terms + place(b, (j >> (block_bit - s - 1)) & 1)
            slot = slot + jnp.where(part == ty, terms, 0)
        pick = jnp.concatenate(
            [jnp.where(slot == lane + c * tile, 1.0, 0.0).astype(BF16) for c in range(orders // tile)], axis=1
        )
        row_load.wait()
        index = lax.broadcasted_iota(jnp.int32, (orders, orders), 0)
        table = jnp.where(index == owner_ref[...], 1.0, 0.0).astype(BF16)
        hot_v[...] = dot_t(pick, table).astype(BF16)

    def whole(ref, sem):
        return pltpu.make_async_copy(ref, ref, sem)

    def gather_copy(ty, t, p, variant):
        return pltpu.make_async_remote_copy(
            src_ref=send0.at[ty, t, p - 1],
            dst_ref=recv0.at[ty, t, p - 1],
            send_sem=sent_sems.at[0],
            recv_sem=sems0.at[t % SLOTS, ty],
            device_id=at(gather[variant][ty][p]),
            device_id_type=MESH,
        )

    def coef_copy(variant, ty, p):
        return pltpu.make_async_remote_copy(
            src_ref=coef_send.at[variant, ty, p - 1],
            dst_ref=coef_recv.at[variant, ty, p - 1],
            send_sem=sent_sems.at[1],
            recv_sem=coef_sems.at[variant, ty],
            device_id=at(gather[variant][ty][p]),
            device_id_type=MESH,
        )

    swap_from = chunks - SWAPPED
    groups = block // GROUP

    def half_copy(s, ty, t):
        partner = flip(me, [later[ty][s]])
        if s < 2:
            partner = jnp.where(t < swap_from, partner, flip(me, [later[ty][1 - s]]))
        if s == 0:
            partner = jnp.where(t == CROSS, flip(me, [FIRST[ty]]), partner)
        return pltpu.make_async_remote_copy(
            src_ref=halves[2 * s].at[ty, t],
            dst_ref=halves[2 * s + 1].at[ty, t],
            send_sem=sent_sems.at[2 + s],
            recv_sem=half_sems.at[s, t % SLOTS, ty],
            device_id=at(partner),
            device_id_type=MESH,
        )

    def enter():
        with jax.named_scope("barrier"):
            pl.semaphore_wait(barrier, len(near))

    def permute(t, variant=0, entered=False):
        with jax.named_scope("load"):
            load(t).wait()
        with jax.named_scope("permute"):
            permute_loaded(t, variant)
        if entered:
            enter()
        for p in (2, 3, 1):
            for ty in range(2):
                gather_copy(ty, t, p, variant).start()

        @pl.when(t + 4 < chunks)
        def _():
            load(t + 4).start()

    def permute_loaded(t, variant):
        together = max(1, 256 // width)
        for r0 in range(0, cycles, together):
            values = jnp.concatenate([leg_v[t, r0 + i] for i in range(together)], axis=1)
            for ty in range(2):
                picked = dot(hot_v[ty * 4 * block : (ty + 1) * 4 * block, :], values).astype(BF16)
                for i in range(together):
                    piece = picked[:, i * width : (i + 1) * width]
                    for p in range(4):
                        rows = [group_row(variant, p, g) for g in range(groups)]
                        rows = jnp.concatenate([piece[row : row + GROUP] for row in rows], axis=0)
                        if p == 0:
                            own0[ty, t, r0 + i] = rows
                        else:
                            send0[ty, t, p - 1, r0 + i] = rows

    permute(0, entered=True)
    permute(CROSS, 1)
    order_load = pltpu.make_async_copy(owner_hbm, owner_smem, table_sem.at[4])
    order_load.start()

    with jax.named_scope("waitsky"):
        whole(sky_v, sky_sem).wait()
    for table in tables:
        table.wait()
    count = maps * cycles
    columns = 2 * orders
    stages = []
    first = first_v[...]
    for b in range(count):
        stage = jnp.dot(
            first, sky_v[b // cycles, b % cycles], precision=lax.Precision.HIGHEST, preferred_element_type=F32
        )
        stages.append(jnp.concatenate([stage[:coarse], stage[coarse:]], axis=1))
    left_high, left_low = split_bf16(jnp.concatenate(stages, axis=0))
    spectral = []
    span = orders // 2
    for c in range(columns // span):
        picked = slice(c * span, (c + 1) * span)
        full = dot(left_high, high_v[:, picked]) + (dot(left_high, low_v[:, picked]) + dot(left_low, high_v[:, picked]))
        full = full.reshape(count, coarse, span)
        m1 = lax.broadcasted_iota(jnp.int32, (1, coarse, span), 1)
        col = lax.broadcasted_iota(jnp.int32, (1, coarse, span), 2)
        spectral.append(jnp.sum(jnp.where(col % coarse == m1, full, 0.0), axis=1))
    spectral = jnp.concatenate(
        [jnp.concatenate(spectral[:2], axis=1), jnp.concatenate(spectral[2:], axis=1)], axis=0
    ).astype(BF16)
    copies = tile // (2 * count)
    coef = dot_t(hot_v[...], jnp.concatenate([spectral] * copies, axis=0))
    lane_group = lax.broadcasted_iota(jnp.int32, (GROUP, tile), 1) // (2 * count)
    for variant in range(2):
        for ty in range(2):
            for p in range(4):
                packed = None
                for g in range(groups):
                    row = ty * 4 * block + group_row(variant, p, g)
                    rows = coef[row : row + GROUP]
                    packed = rows if packed is None else jnp.where(lane_group == g, rows, packed)
                if p == 0:
                    coef_own[variant, ty] = packed.astype(BF16)
                else:
                    coef_send[variant, ty, p - 1] = packed.astype(BF16)
    for variant in range(2):
        for p in (2, 3, 1):
            for ty in range(2):
                coef_copy(variant, ty, p).start()

    order_load.wait()

    def permute_step(t, carry):
        permute(t)
        return carry

    lax.fori_loop(CROSS + 1, AHEAD + 1, permute_step, 0)

    source = lax.broadcasted_iota(jnp.int32, (tile, cycles * tile), 0)
    target = lax.broadcasted_iota(jnp.int32, (tile, cycles * tile), 1)
    channel = 2 * ((source // cycles) % maps) + (source // count) % 2
    same = (source % cycles == target // tile) & (channel == target % channels)
    expand = jnp.where(same, 1.0, 0.0).astype(BF16)
    depth = 4 * cycles * GROUP
    keep = lax.broadcasted_iota(jnp.int32, (depth, tile), 0) % GROUP == (
        lax.broadcasted_iota(jnp.int32, (depth, tile), 1) // channels
    )
    pack_group = lax.broadcasted_iota(jnp.int32, (4 * GROUP, tile), 1) // (2 * count)

    def build(variant):
        for ty in range(2):
            with scope("waitcoef"):
                whole(coef_recv.at[variant, ty], coef_sems.at[variant, ty]).wait()
            values = [coef_own[variant, ty]] + [coef_recv[variant, ty, p] for p in range(3)]
            values = jnp.concatenate(values, axis=0).astype(F32)
            for g in range(groups):
                spread = dot(jnp.where(pack_group == g, values, 0.0).astype(BF16), expand)
                pieces = [
                    spread[p * GROUP : (p + 1) * GROUP, r * tile : (r + 1) * tile]
                    for p in range(4)
                    for r in range(cycles)
                ]
                stacked = jnp.where(keep, jnp.concatenate(pieces, axis=0), 0.0)
                lhs_v[variant, ty, g] = stacked.T.astype(BF16)

    build(0)
    high_rows = GROUP * channels

    def product(variant, ty, t, g):
        span = slice(g * GROUP, (g + 1) * GROUP)
        parts = [own0[ty, t, :, span, :]] + [recv0[ty, t, p, :, span, :] for p in range(3)]
        right = jnp.concatenate([v.reshape(cycles * GROUP, width) for v in parts], axis=0)
        return dot(lhs_v[variant, ty, g], right)

    def first_step(t, sent, kept, variant=0):
        for ty in range(2):
            with jax.named_scope("wait0"):
                whole(recv0.at[ty, t], sems0.at[t % SLOTS, ty]).wait()
            for i, g in enumerate(sent):
                halves[0][ty, t, i * high_rows : (i + 1) * high_rows, :] = product(variant, ty, t, g).astype(BF16)
            half_copy(0, ty, t).start()
        for ty in range(2):
            for i, g in enumerate(kept):
                acc_v[ty, t, i * high_rows : (i + 1) * high_rows, :] = product(variant, ty, t, g)

    def next_step(s, t):
        size = rows0 >> (s + 1)
        for ty in range(2):
            with jax.named_scope(f"wait{s}"):
                half_copy(s - 1, ty, t).wait_recv()
            got = halves[2 * s - 1]
            value = acc_v[ty, t, size : 2 * size, :] + got[ty, t, size:, :].astype(F32)
            halves[2 * s][ty, t] = value.astype(BF16)
            half_copy(s, ty, t).start()
            acc_v[ty, t, :size, :] = acc_v[ty, t, :size, :] + got[ty, t, :size, :].astype(F32)

    def pow_copy(u):
        return pltpu.make_async_remote_copy(
            src_ref=pow_v.at[u],
            dst_ref=pow_recv.at[me // sharers],
            send_sem=sent_sems.at[2 + steps],
            recv_sem=pow_sem,
            device_id=at(u * sharers + me % sharers),
            device_id_type=MESH,
        )

    def last_step(t):
        size = rows0 >> steps
        ell = place_of(t) * width + lax.broadcasted_iota(jnp.int32, (channels, width), 1)
        total = [None] * (maps // 2 + 1)
        lanes = pl.ds(pl.multiple_of(place_of(t) * width, width), width)
        for ty in range(2):
            with jax.named_scope("waitlast"):
                half_copy(steps - 1, ty, t).wait_recv()
            value = acc_v[ty, t, :size, :] + halves[2 * steps - 1][ty, t].astype(F32)
            for i in range(per_type):
                order = owner_smem[me * own + ty * per_type + i]
                mode = jnp.where(ell >= order, value[i * channels : (i + 1) * channels], 0.0)
                row = (ty * per_type + i) * maps
                for a in range(maps):
                    harm_ref[row + a, :, lanes] = mode[2 * a : 2 * a + 2]
                heavy = mode * jnp.where(order == 0, 1.0, 2.0)
                for k in range(maps // 2 + 1):
                    turned = mode if k == 0 else jnp.concatenate([mode[2 * k :], mode[: 2 * k]], axis=0)
                    term = heavy * turned
                    total[k] = term if total[k] is None else total[k] + term
        rows = []
        for i in range(maps):
            for jj in range(i, maps):
                k, a = (jj - i, i) if jj - i <= maps // 2 else (maps - (jj - i), jj)
                rows.append(total[k][2 * a : 2 * a + 1] + total[k][2 * a + 1 : 2 * a + 2])
        power = jnp.concatenate(rows, axis=0)
        for h in range(width // tile):
            u = place_of(t) * (width // tile) + h
            pow_v[u] = power[:, h * tile : (h + 1) * tile]

            @pl.when(u != me // sharers)
            def _():
                pow_copy(u).start()

    lags = [0, LAGS[0]]
    for s in range(2, steps):
        lags.append(lags[-1] + LAGS[1])
    end = lags[-1] + LAGS[2]

    def first_of(t):
        @pl.when((t < swap_from) & (t != CROSS))
        def _():
            with scope("first"):
                first_step(t, (2, 3), (0, 1))

        @pl.when(t == CROSS)
        def _():
            with scope("build"):
                build(1)
            with scope("first"):
                first_step(t, (2, 3), (0, 1), 1)

        @pl.when((t >= swap_from) & (t < chunks))
        def _():
            with scope("first"):
                first_step(t, (1, 3), (0, 2))

    def later_of(t):
        for s in range(1, steps):

            @pl.when((t >= lags[s]) & (t < chunks + lags[s]))
            def _():
                with scope(f"next{s}"):
                    next_step(s, t - lags[s])

        @pl.when(t >= end)
        def _():
            with scope("last"):
                last_step(t - end)

    def main(t, carry):
        @pl.when((t > 0) & (t + AHEAD < chunks))
        def _():
            permute(t + AHEAD)

        first_of(t)
        later_of(t)
        return carry

    special = steps == 3 and chunks >= 14
    lax.fori_loop(0, chunks - 2 if special else chunks + end, main, 0)
    if special:
        with scope("finale"):
            for e, back in FINALE:
                t = chunks - back
                with scope(f"e{e}"):
                    if e == 0:
                        first_step(t, (1, 3) if back <= SWAPPED else (2, 3), (0, 2) if back <= SWAPPED else (0, 1))
                    elif e < 3:
                        next_step(e, t)
                    else:
                        last_step(t)

    mine = me // sharers
    total = pow_v[mine]
    with scope("waitpow"):
        whole(pow_recv.at[: tiles - 1], pow_sem).wait()
    for u in range(tiles):
        total = total + jnp.where(u != mine, pow_recv[u], 0.0)
    pow_mine[...] = total

    def pair_copy(e):
        return pltpu.make_async_remote_copy(
            src_ref=pow_mine,
            dst_ref=pow_pair.at[e - 1],
            send_sem=pair_sems.at[0, e - 1],
            recv_sem=pair_sems.at[1, e - 1],
            device_id=at(mine * sharers + (me + e) % sharers),
            device_id_type=MESH,
        )

    for e in range(1, sharers):
        pair_copy(e).start()
    for e in range(1, sharers):
        with jax.named_scope("waitpair"):
            pair_copy(e).wait_recv()
        total = total + pow_pair[e - 1]
    ell = mine * tile + lax.broadcasted_iota(jnp.int32, total.shape, 1)
    total = total / (2 * ell + 1).astype(F32)
    share = tile // sharers
    turned = total
    for c in range(1, sharers):
        shifted = jnp.concatenate([total[:, c * share :], total[:, : c * share]], axis=1)
        turned = jnp.where(me % sharers == c, shifted, turned)
    spec_ref[...] = turned[:, :share]

    with jax.named_scope("drain"):
        whole(send0, sent_sems.at[0]).wait()
        whole(coef_send, sent_sems.at[1]).wait()
        for s in range(steps):
            whole(halves[2 * s], sent_sems.at[2 + s]).wait()
    for e in range(1, sharers):
        pair_copy(e).wait_send()
    whole(pow_v.at[: tiles - 1], sent_sems.at[2 + steps]).wait()


def hand_over_body(large_ref, small_ref, large_out, small_out, sems):
    copies = [
        pltpu.make_async_copy(large_ref, large_out, sems.at[0]),
        pltpu.make_async_copy(small_ref, small_out, sems.at[1]),
    ]
    for copy in copies:
        copy.start()
    for copy in copies:
        copy.wait()


def hand_over(large, small):
    return pl.pallas_call(
        hand_over_body,
        out_shape=[jax.ShapeDtypeStruct(large.shape, large.dtype), jax.ShapeDtypeStruct(small.shape, small.dtype)],
        in_specs=[pl.BlockSpec(memory_space=pltpu.VMEM)] * 2,
        out_specs=[pl.BlockSpec(memory_space=pl.ANY)] * 2,
        scratch_shapes=[pltpu.SemaphoreType.DMA((2,))],
        cost_estimate=pl.CostEstimate(flops=large.size, bytes_accessed=8 * large.size, transcendentals=0),
    )(large, small)


def per_device(sky_maps, legendre, owner_table):
    maps, cycles, pixels = sky_maps.shape
    _, orders, ells = legendre.shape
    devices = lax.axis_size(AXES)
    grp = lax.axis_size(AXES[1])
    bits = devices.bit_length() - 1
    steps = bits - 2
    width = WIDTH
    chunks = ells // width
    channels = 2 * maps
    own = orders // devices
    block = orders // 8
    tile = 128
    coarse = pixels // tile
    tiles = ells // tile
    sharers = tile * devices // ells
    pairs = maps * (maps + 1) // 2
    first, high, low = fourier_tables(pixels, orders, tile)
    rows0 = block * channels
    halves = []
    for s in range(steps):
        halves += [pltpu.VMEM((2, chunks, rows0 >> (s + 1), width), BF16)] * 2
    cfg = (maps, cycles, orders, ells, devices, grp, width)
    scratch = [
        pltpu.SMEM((orders,), jnp.int32),
        pltpu.VMEM((1, orders), jnp.int32),
        pltpu.VMEM((orders, tile), F32),
        pltpu.VMEM((chunks, cycles, orders, width), BF16),
        pltpu.VMEM((maps, cycles, coarse, tile), F32),
        pltpu.VMEM(first.shape, F32),
        pltpu.VMEM(high.shape, BF16),
        pltpu.VMEM(low.shape, BF16),
        pltpu.VMEM((orders, orders), BF16),
        pltpu.VMEM((2, 2, block // GROUP, GROUP * channels, 4 * cycles * GROUP), BF16),
        pltpu.VMEM((2, chunks, cycles, block, width), BF16),
        pltpu.VMEM((2, chunks, 3, cycles, block, width), BF16),
        pltpu.VMEM((2, chunks, 3, cycles, block, width), BF16),
        pltpu.VMEM((2, 2, GROUP, tile), BF16),
        pltpu.VMEM((2, 2, 3, GROUP, tile), BF16),
        pltpu.VMEM((2, 2, 3, GROUP, tile), BF16),
        pltpu.VMEM((2, chunks, rows0 // 2, width), F32),
        halves,
        pltpu.VMEM((tiles, pairs, tile), F32),
        pltpu.VMEM((tiles, pairs, tile), F32),
        pltpu.VMEM((pairs, tile), F32),
        pltpu.VMEM((sharers - 1, pairs, tile), F32),
        pltpu.SemaphoreType.DMA((4,)),
        pltpu.SemaphoreType.DMA,
        pltpu.SemaphoreType.DMA((5,)),
        pltpu.SemaphoreType.DMA((3 + steps,)),
        pltpu.SemaphoreType.DMA((SLOTS, 2)),
        pltpu.SemaphoreType.DMA((2, 2)),
        pltpu.SemaphoreType.DMA((steps, SLOTS, 2)),
        pltpu.SemaphoreType.DMA,
        pltpu.SemaphoreType.DMA((2, sharers - 1)),
    ]
    anywhere = pl.BlockSpec(memory_space=pl.ANY)
    vmem = pl.BlockSpec(memory_space=pltpu.VMEM)
    harmonics, spectra = pl.pallas_call(
        functools.partial(kernel, cfg),
        out_shape=[
            pltpu.VMEM((own * maps, 2, ells), F32),
            pltpu.VMEM((pairs, ells // devices), F32),
        ],
        in_specs=[anywhere] * 7,
        out_specs=[vmem, vmem],
        scratch_shapes=scratch,
        compiler_params=pltpu.CompilerParams(
            vmem_limit_bytes=56 * MIB, collective_id=0, has_side_effects=True
        ),
        cost_estimate=pl.CostEstimate(
            flops=2 * cycles * orders * orders * ells, bytes_accessed=2 * legendre.size, transcendentals=0
        ),
    )(
        owner_table,
        owner_table.reshape(1, orders),
        sky_maps,
        jnp.asarray(first),
        jnp.asarray(high),
        jnp.asarray(low),
        legendre,
    )
    harmonics, spectra = (pltpu.with_memory_space_constraint(v, pltpu.VMEM) for v in (harmonics, spectra))
    harmonics, spectra = hand_over(harmonics, spectra)
    return harmonics.reshape(own, maps, 2, ells), spectra


def solution(mesh):
    return jax.shard_map(
        per_device,
        mesh=mesh,
        in_specs=(P(None, AXES, None), P(AXES, None, None), P()),
        out_specs=(P(AXES, None, None, None), P(None, AXES)),
        check_vma=False,
    )
```

```python
import functools
import math

import jax
import jax.numpy as jnp
import numpy as np
from jax import lax
from jax.experimental import pallas as pl
from jax.experimental.pallas import tpu as pltpu
from jax.sharding import PartitionSpec as P

AXES = ("blk", "grp")
MIB = 1024 * 1024
MESH = pl.DeviceIdType.MESH
BF16 = jnp.bfloat16
F32 = jnp.float32
GROUP = 16
FIRST = (1, 2)
EARLY = 3
WIDTH = 128
AHEAD = 3
CROSS = 1
SWAPPED = 1
FINALE = (
    *((1, 4), (0, 2), (3, 9), (3, 8), (1, 3), (0, 1), (2, 6), (2, 5), (3, 7), (2, 4), (2, 3)),
    *((1, 2), (1, 1), (3, 6), (2, 2), (3, 5), (2, 1), (3, 4), (3, 3), (3, 2), (3, 1)),
)
ROTATE = 0
SLOTS = 8
LAGS = (2, 2, 3)


def plan_of(bits):
    later = [[EARLY] + [b for b in range(1, bits) if b not in (first, EARLY)] for first in FIRST]
    return later


def flip(me, bits):
    out = me
    for b in bits:
        out = out + (1 - 2 * ((me // (1 << b)) % 2)) * (1 << b)
    return out


def split_bf16(values):
    high = values.astype(BF16)
    low = (values - high.astype(F32)).astype(BF16)
    return high, low


def dot(left, right):
    return jnp.dot(left, right, preferred_element_type=F32)


def dot_t(left, right):
    return lax.dot_general(left, right, (((1,), (1,)), ((), ())), preferred_element_type=F32)


def fourier_tables(pixels, order_count, width):
    coarse = pixels // width
    k1, m1 = np.meshgrid(np.arange(coarse), np.arange(coarse), indexing="ij")
    angle = 2.0 * math.pi * ((k1 * m1) % coarse) / coarse
    first = np.concatenate([np.cos(angle.T), -np.sin(angle.T)], axis=0)
    k2 = np.arange(width)[:, None]
    m = np.arange(order_count)[None, :]
    angle = 2.0 * math.pi * ((k2 * m) % pixels) / pixels
    cosine, sine = np.cos(angle) / math.sqrt(pixels), np.sin(angle) / math.sqrt(pixels)
    second = np.block([[cosine, -sine], [sine, cosine]]).astype(np.float32)
    high = second.astype(jnp.bfloat16)
    low = (second - high.astype(np.float32)).astype(jnp.bfloat16)
    return first.astype(np.float32), high, low


def kernel(
    cfg, owner_hbm, owner_row_hbm, sky_hbm, first_hbm, high_hbm, low_hbm, leg_hbm, harm_ref, spec_ref,
    owner_smem, owner_ref, column_v, leg_v, sky_v, first_v, high_v, low_v, hot_v, lhs_v, own0, send0, recv0, coef_own, coef_send, coef_recv,
    acc_v, halves, pow_v, pow_recv, pow_mine, pow_pair, pow_total, pow_direct, load_sem, sky_sem, table_sem,
    sent_sems, sems0, coef_sems, half_sems, pow_sems, pair_sems,
):
    maps, cycles, orders, ells, devices, grp, width = cfg
    bits = devices.bit_length() - 1
    later = plan_of(bits)
    steps = bits - 2
    chunks = ells // width
    channels = 2 * maps
    own = orders // devices
    per_type = own // 2
    block = orders // 8
    rows0 = block * channels
    me = lax.axis_index("blk") * grp + lax.axis_index("grp")
    tile = 128
    tiles = ells // tile
    sharers = tile * devices // ells
    pairs = maps * (maps + 1) // 2

    def at(index):
        return (index // grp, index % grp)

    def bit(b):
        return (me // (1 << b)) % 2

    gather = [
        [[None, flip(me, [0]), flip(me, [b]), flip(me, [b, 0])] for b in firsts] for firsts in (FIRST, (EARLY, EARLY))
    ]
    near = sorted({(b,) for b in range(bits)} | {(0, b) for b in FIRST + (EARLY,)}, reverse=True)

    def group_row(variant, p, g):
        q = p * 4 + g if variant == 0 else (g // 2) * 8 + (p % 2) * 4 + (p // 2) * 2 + g % 2
        return q * GROUP

    scope = jax.named_scope
    row_load = pltpu.make_async_copy(owner_row_hbm, owner_ref, table_sem.at[3])
    row_load.start()
    barrier = pltpu.get_barrier_semaphore()
    for masks in near:
        pl.semaphore_signal(barrier, inc=1, device_id=at(flip(me, masks)), device_id_type=MESH)

    def place_of(t):
        return (t + ROTATE * chunks // 16) % chunks

    def load(t):
        lanes = pl.ds(pl.multiple_of(place_of(t) * width, width), width)
        return pltpu.make_async_copy(leg_hbm.at[:, :, lanes], leg_v.at[t], load_sem.at[t % 4])

    def load_start(t, carry):
        load(t).start()
        return carry

    with scope("startload"):
        lax.fori_loop(0, 4, load_start, 0)
    coarse = sky_v.shape[2]

    def sky_load(k):
        lanes = pl.ds(k * tile, tile)
        return pltpu.make_async_copy(sky_hbm.at[:, :, lanes], sky_v.at[:, :, k, :], sky_sem)

    for k in range(coarse):
        sky_load(k).start()
    tables = [
        pltpu.make_async_copy(src, dst, table_sem.at[i])
        for i, (src, dst) in enumerate(((first_hbm, first_v), (high_hbm, high_v), (low_hbm, low_v)))
    ]
    for table in tables:
        table.start()


    half_bit, block_bit = (orders // 2).bit_length() - 1, block.bit_length() - 1

    def place(b, differs):
        mine = bit(b)
        return (mine + differs - 2 * mine * differs) * ((1 << b) * own)

    lane = lax.broadcasted_iota(jnp.int32, (orders, tile), 1)
    if per_type % 8 == 0:
        places = [[place(b, differs) for differs in range(2)] for b in range(bits)]
        row_load.wait()
        for c in range(orders // tile):
            row = owner_ref[:, c * tile : (c + 1) * tile].astype(F32)
            column_v[c * tile : (c + 1) * tile, :] = jnp.broadcast_to(row, (tile, tile)).T
        picked = []
        for jb in range(0, orders, 8):
            ty = jb >> half_bit
            start = ty * per_type + jb % per_type + places[0][(jb >> block_bit) & 1]
            start = start + places[FIRST[ty]][(jb >> (block_bit + 1)) & 1]
            for s, b in enumerate(later[ty]):
                start = start + places[b][(jb >> (block_bit - s - 1)) & 1]
            picked.append(column_v[pl.ds(pl.multiple_of(start, 8), 8), :])
        column = jnp.concatenate(picked, axis=0)
        lane = lane.astype(F32)
        for c in range(orders // tile):
            hot_v[:, c * tile : (c + 1) * tile] = jnp.where(column == lane + float(c * tile), 1.0, 0.0).astype(BF16)
    else:
        j = lax.broadcasted_iota(jnp.int32, (orders, tile), 0)
        part = j >> half_bit
        slot = part * per_type + (j & (per_type - 1)) + place(0, (j >> block_bit) & 1)
        for ty in range(2):
            terms = place(FIRST[ty], (j >> (block_bit + 1)) & 1)
            for s, b in enumerate(later[ty]):
                terms = terms + place(b, (j >> (block_bit - s - 1)) & 1)
            slot = slot + jnp.where(part == ty, terms, 0)
        pick = jnp.concatenate(
            [jnp.where(slot == lane + c * tile, 1.0, 0.0).astype(BF16) for c in range(orders // tile)], axis=1
        )
        row_load.wait()
        index = lax.broadcasted_iota(jnp.int32, (orders, orders), 0)
        table = jnp.where(index == owner_ref[...], 1.0, 0.0).astype(BF16)
        hot_v[...] = dot_t(pick, table).astype(BF16)

    def whole(ref, sem):
        return pltpu.make_async_copy(ref, ref, sem)

    def gather_copy(ty, t, p, variant):
        return pltpu.make_async_remote_copy(
            src_ref=send0.at[ty, t, p - 1],
            dst_ref=recv0.at[ty, t, p - 1],
            send_sem=sent_sems.at[0],
            recv_sem=sems0.at[t % SLOTS, ty],
            device_id=at(gather[variant][ty][p]),
            device_id_type=MESH,
        )

    def coef_copy(variant, ty, p):
        return pltpu.make_async_remote_copy(
            src_ref=coef_send.at[variant, ty, p - 1],
            dst_ref=coef_recv.at[variant, ty, p - 1],
            send_sem=sent_sems.at[1],
            recv_sem=coef_sems.at[variant, ty],
            device_id=at(gather[variant][ty][p]),
            device_id_type=MESH,
        )

    swap_from = chunks - SWAPPED
    groups = block // GROUP

    def half_copy(s, ty, t):
        partner = flip(me, [later[ty][s]])
        if s < 2:
            partner = jnp.where(t < swap_from, partner, flip(me, [later[ty][1 - s]]))
        if s == 0:
            partner = jnp.where(t == CROSS, flip(me, [FIRST[ty]]), partner)
        return pltpu.make_async_remote_copy(
            src_ref=halves[2 * s].at[ty, t],
            dst_ref=halves[2 * s + 1].at[ty, t],
            send_sem=sent_sems.at[2 + s],
            recv_sem=half_sems.at[s, t % SLOTS, ty],
            device_id=at(partner),
            device_id_type=MESH,
        )

    def enter():
        with jax.named_scope("barrier"):
            pl.semaphore_wait(barrier, len(near))

    def permute(t, variant=0, entered=False):
        with jax.named_scope("load"):
            load(t).wait()
        with jax.named_scope("permute"):
            permute_loaded(t, variant)
        if entered:
            enter()
        for p in (2, 3, 1):
            for ty in range(2):
                gather_copy(ty, t, p, variant).start()

        @pl.when(t + 4 < chunks)
        def _():
            load(t + 4).start()

    def permute_loaded(t, variant):
        together = max(1, 256 // width)
        for r0 in range(0, cycles, together):
            values = jnp.concatenate([leg_v[t, r0 + i] for i in range(together)], axis=1)
            for ty in range(2):
                picked = dot(hot_v[ty * 4 * block : (ty + 1) * 4 * block, :], values).astype(BF16)
                for i in range(together):
                    piece = picked[:, i * width : (i + 1) * width]
                    for p in range(4):
                        rows = [group_row(variant, p, g) for g in range(groups)]
                        rows = jnp.concatenate([piece[row : row + GROUP] for row in rows], axis=0)
                        if p == 0:
                            own0[ty, t, r0 + i] = rows
                        else:
                            send0[ty, t, p - 1, r0 + i] = rows

    permute(0, entered=True)
    permute(CROSS, 1)
    order_load = pltpu.make_async_copy(owner_hbm, owner_smem, table_sem.at[4])
    order_load.start()

    with jax.named_scope("waitsky"):
        whole(sky_v, sky_sem).wait()
    for table in tables:
        table.wait()
    count = maps * cycles
    columns = 2 * orders
    stages = []
    first = first_v[...]
    for b in range(count):
        stage = jnp.dot(
            first, sky_v[b // cycles, b % cycles], precision=lax.Precision.HIGHEST, preferred_element_type=F32
        )
        stages.append(jnp.concatenate([stage[:coarse], stage[coarse:]], axis=1))
    left_high, left_low = split_bf16(jnp.concatenate(stages, axis=0))
    spectral = []
    span = orders // 2
    for c in range(columns // span):
        picked = slice(c * span, (c + 1) * span)
        full = dot(left_high, high_v[:, picked]) + (dot(left_high, low_v[:, picked]) + dot(left_low, high_v[:, picked]))
        full = full.reshape(count, coarse, span)
        m1 = lax.broadcasted_iota(jnp.int32, (1, coarse, span), 1)
        col = lax.broadcasted_iota(jnp.int32, (1, coarse, span), 2)
        spectral.append(jnp.sum(jnp.where(col % coarse == m1, full, 0.0), axis=1))
    spectral = jnp.concatenate(
        [jnp.concatenate(spectral[:2], axis=1), jnp.concatenate(spectral[2:], axis=1)], axis=0
    ).astype(BF16)
    copies = tile // (2 * count)
    coef = dot_t(hot_v[...], jnp.concatenate([spectral] * copies, axis=0))
    lane_group = lax.broadcasted_iota(jnp.int32, (GROUP, tile), 1) // (2 * count)
    for variant in range(2):
        for ty in range(2):
            for p in range(4):
                packed = None
                for g in range(groups):
                    row = ty * 4 * block + group_row(variant, p, g)
                    rows = coef[row : row + GROUP]
                    packed = rows if packed is None else jnp.where(lane_group == g, rows, packed)
                if p == 0:
                    coef_own[variant, ty] = packed.astype(BF16)
                else:
                    coef_send[variant, ty, p - 1] = packed.astype(BF16)
    for variant in range(2):
        for p in (2, 3, 1):
            for ty in range(2):
                coef_copy(variant, ty, p).start()

    order_load.wait()

    def permute_step(t, carry):
        permute(t)
        return carry

    lax.fori_loop(CROSS + 1, AHEAD + 1, permute_step, 0)

    source = lax.broadcasted_iota(jnp.int32, (tile, cycles * tile), 0)
    target = lax.broadcasted_iota(jnp.int32, (tile, cycles * tile), 1)
    channel = 2 * ((source // cycles) % maps) + (source // count) % 2
    same = (source % cycles == target // tile) & (channel == target % channels)
    expand = jnp.where(same, 1.0, 0.0).astype(BF16)
    depth = 4 * cycles * GROUP
    keep = lax.broadcasted_iota(jnp.int32, (depth, tile), 0) % GROUP == (
        lax.broadcasted_iota(jnp.int32, (depth, tile), 1) // channels
    )
    pack_group = lax.broadcasted_iota(jnp.int32, (4 * GROUP, tile), 1) // (2 * count)

    def build(variant):
        for ty in range(2):
            with scope("waitcoef"):
                whole(coef_recv.at[variant, ty], coef_sems.at[variant, ty]).wait()
            values = [coef_own[variant, ty]] + [coef_recv[variant, ty, p] for p in range(3)]
            values = jnp.concatenate(values, axis=0).astype(F32)
            for g in range(groups):
                spread = dot(jnp.where(pack_group == g, values, 0.0).astype(BF16), expand)
                pieces = [
                    spread[p * GROUP : (p + 1) * GROUP, r * tile : (r + 1) * tile]
                    for p in range(4)
                    for r in range(cycles)
                ]
                stacked = jnp.where(keep, jnp.concatenate(pieces, axis=0), 0.0)
                lhs_v[variant, ty, g] = stacked.T.astype(BF16)

    build(0)
    high_rows = GROUP * channels

    def product(variant, ty, t, g):
        span = slice(g * GROUP, (g + 1) * GROUP)
        parts = [own0[ty, t, :, span, :]] + [recv0[ty, t, p, :, span, :] for p in range(3)]
        right = jnp.concatenate([v.reshape(cycles * GROUP, width) for v in parts], axis=0)
        return dot(lhs_v[variant, ty, g], right)

    def first_step(t, sent, kept, variant=0):
        for ty in range(2):
            with jax.named_scope("wait0"):
                whole(recv0.at[ty, t], sems0.at[t % SLOTS, ty]).wait()
            for i, g in enumerate(sent):
                halves[0][ty, t, i * high_rows : (i + 1) * high_rows, :] = product(variant, ty, t, g).astype(BF16)
            half_copy(0, ty, t).start()
        for ty in range(2):
            for i, g in enumerate(kept):
                acc_v[ty, t, i * high_rows : (i + 1) * high_rows, :] = product(variant, ty, t, g)

    def next_step(s, t):
        size = rows0 >> (s + 1)
        for ty in range(2):
            with jax.named_scope(f"wait{s}"):
                half_copy(s - 1, ty, t).wait_recv()
            got = halves[2 * s - 1]
            value = acc_v[ty, t, size : 2 * size, :] + got[ty, t, size:, :].astype(F32)
            halves[2 * s][ty, t] = value.astype(BF16)
            half_copy(s, ty, t).start()
            acc_v[ty, t, :size, :] = acc_v[ty, t, :size, :] + got[ty, t, :size, :].astype(F32)

    def pow_copy(u):
        return pltpu.make_async_remote_copy(
            src_ref=pow_v.at[u],
            dst_ref=pow_recv.at[me // sharers],
            send_sem=sent_sems.at[2 + steps],
            recv_sem=pow_sems.at[0],
            device_id=at(u * sharers + me % sharers),
            device_id_type=MESH,
        )

    def direct_copy(u, owner):
        return pltpu.make_async_remote_copy(
            src_ref=pow_v.at[u],
            dst_ref=pow_direct.at[me],
            send_sem=sent_sems.at[3 + steps],
            recv_sem=pow_sems.at[1],
            device_id=at(owner),
            device_id_type=MESH,
        )

    def last_step(t, direct=False):
        size = rows0 >> steps
        ell = place_of(t) * width + lax.broadcasted_iota(jnp.int32, (channels, width), 1)
        total = [None] * (maps // 2 + 1)
        lanes = pl.ds(pl.multiple_of(place_of(t) * width, width), width)
        for ty in range(2):
            with jax.named_scope("waitlast"):
                half_copy(steps - 1, ty, t).wait_recv()
            value = acc_v[ty, t, :size, :] + halves[2 * steps - 1][ty, t].astype(F32)
            for i in range(per_type):
                order = owner_smem[me * own + ty * per_type + i]
                mode = jnp.where(ell >= order, value[i * channels : (i + 1) * channels], 0.0)
                row = (ty * per_type + i) * maps
                for a in range(maps):
                    harm_ref[row + a, :, lanes] = mode[2 * a : 2 * a + 2]
                heavy = mode * jnp.where(order == 0, 1.0, 2.0)
                for k in range(maps // 2 + 1):
                    turned = mode if k == 0 else jnp.concatenate([mode[2 * k :], mode[: 2 * k]], axis=0)
                    term = heavy * turned
                    total[k] = term if total[k] is None else total[k] + term
        rows = []
        for i in range(maps):
            for jj in range(i, maps):
                k, a = (jj - i, i) if jj - i <= maps // 2 else (maps - (jj - i), jj)
                rows.append(total[k][2 * a : 2 * a + 1] + total[k][2 * a + 1 : 2 * a + 2])
        power = jnp.concatenate(rows, axis=0)
        for h in range(width // tile):
            u = place_of(t) * (width // tile) + h
            pow_v[u] = power[:, h * tile : (h + 1) * tile]

            if direct:
                for e in range(sharers):

                    @pl.when(u * sharers + e != me)
                    def _():
                        direct_copy(u, u * sharers + e).start()

            else:

                @pl.when(u != me // sharers)
                def _():
                    pow_copy(u).start()

    lags = [0, LAGS[0]]
    for s in range(2, steps):
        lags.append(lags[-1] + LAGS[1])
    end = lags[-1] + LAGS[2]

    def first_of(t):
        @pl.when((t < swap_from) & (t != CROSS))
        def _():
            with scope("first"):
                first_step(t, (2, 3), (0, 1))

        @pl.when(t == CROSS)
        def _():
            with scope("build"):
                build(1)
            with scope("first"):
                first_step(t, (2, 3), (0, 1), 1)

        @pl.when((t >= swap_from) & (t < chunks))
        def _():
            with scope("first"):
                first_step(t, (1, 3), (0, 2))

    def later_of(t):
        for s in range(1, steps):

            @pl.when((t >= lags[s]) & (t < chunks + lags[s]))
            def _():
                with scope(f"next{s}"):
                    next_step(s, t - lags[s])

        @pl.when(t >= end)
        def _():
            with scope("last"):
                last_step(t - end)

    def main(t, carry):
        @pl.when((t > 0) & (t + AHEAD < chunks))
        def _():
            permute(t + AHEAD)

        first_of(t)
        later_of(t)
        return carry

    special = steps == 3 and chunks >= 14
    lax.fori_loop(0, chunks - 2 if special else chunks + end, main, 0)
    if special:
        with scope("finale"):
            for e, back in FINALE:
                t = chunks - back
                with scope(f"e{e}"):
                    if e == 0:
                        first_step(t, (1, 3) if back <= SWAPPED else (2, 3), (0, 2) if back <= SWAPPED else (0, 1))
                    elif e < 3:
                        next_step(e, t)
                    else:
                        last_step(t, direct=back == 1)

    mine = me // sharers
    straight = (tiles - 1 + ROTATE) % tiles if special else tiles

    def pair_copy(e):
        return pltpu.make_async_remote_copy(
            src_ref=pow_mine,
            dst_ref=pow_pair.at[e - 1],
            send_sem=pair_sems.at[0, e - 1],
            recv_sem=pair_sems.at[1, e - 1],
            device_id=at(mine * sharers + (me + e) % sharers),
            device_id_type=MESH,
        )

    @pl.when(mine != straight)
    def _():
        with scope("waitpow"):
            whole(pow_recv.at[: tiles - 1], pow_sems.at[0]).wait()
        total = pow_v[mine]
        for u in range(tiles):
            total = total + jnp.where(u != mine, pow_recv[u], 0.0)
        pow_mine[...] = total
        for e in range(1, sharers):
            pair_copy(e).start()
        with scope("waitpair"):
            for e in range(1, sharers):
                pair_copy(e).wait_recv()
                total = total + pow_pair[e - 1]
        pow_total[...] = total

    if special:

        @pl.when(mine == straight)
        def _():
            with scope("waitpow"):
                whole(pow_direct.at[: devices - 1], pow_sems.at[1]).wait()
            total = pow_v[mine]
            for d in range(devices):
                total = total + jnp.where(d != me, pow_direct[d], 0.0)
            pow_total[...] = total

    total = pow_total[...]
    ell = mine * tile + lax.broadcasted_iota(jnp.int32, total.shape, 1)
    total = total / (2 * ell + 1).astype(F32)
    share = tile // sharers
    turned = total
    for c in range(1, sharers):
        shifted = jnp.concatenate([total[:, c * share :], total[:, : c * share]], axis=1)
        turned = jnp.where(me % sharers == c, shifted, turned)
    spec_ref[...] = turned[:, :share]

    with jax.named_scope("drain"):
        whole(send0, sent_sems.at[0]).wait()
        whole(coef_send, sent_sems.at[1]).wait()
        for s in range(steps):
            whole(halves[2 * s], sent_sems.at[2 + s]).wait()
    if special:

        @pl.when(mine == straight)
        def _():
            whole(pow_v.at[: tiles - 1], sent_sems.at[2 + steps]).wait()
            whole(pow_v.at[: sharers - 1], sent_sems.at[3 + steps]).wait()

        @pl.when(mine != straight)
        def _():
            whole(pow_v.at[: tiles - 2], sent_sems.at[2 + steps]).wait()
            whole(pow_v.at[:sharers], sent_sems.at[3 + steps]).wait()

    else:
        whole(pow_v.at[: tiles - 1], sent_sems.at[2 + steps]).wait()

    @pl.when(mine != straight)
    def _():
        for e in range(1, sharers):
            pair_copy(e).wait_send()


def hand_over_body(large_ref, small_ref, large_out, small_out, sems):
    copies = [
        pltpu.make_async_copy(large_ref, large_out, sems.at[0]),
        pltpu.make_async_copy(small_ref, small_out, sems.at[1]),
    ]
    for copy in copies:
        copy.start()
    for copy in copies:
        copy.wait()


def hand_over(large, small):
    return pl.pallas_call(
        hand_over_body,
        out_shape=[jax.ShapeDtypeStruct(large.shape, large.dtype), jax.ShapeDtypeStruct(small.shape, small.dtype)],
        in_specs=[pl.BlockSpec(memory_space=pltpu.VMEM)] * 2,
        out_specs=[pl.BlockSpec(memory_space=pl.ANY)] * 2,
        scratch_shapes=[pltpu.SemaphoreType.DMA((2,))],
        cost_estimate=pl.CostEstimate(flops=large.size, bytes_accessed=8 * large.size, transcendentals=0),
    )(large, small)


def per_device(sky_maps, legendre, owner_table):
    maps, cycles, pixels = sky_maps.shape
    _, orders, ells = legendre.shape
    devices = lax.axis_size(AXES)
    grp = lax.axis_size(AXES[1])
    bits = devices.bit_length() - 1
    steps = bits - 2
    width = WIDTH
    chunks = ells // width
    channels = 2 * maps
    own = orders // devices
    block = orders // 8
    tile = 128
    coarse = pixels // tile
    tiles = ells // tile
    sharers = tile * devices // ells
    pairs = maps * (maps + 1) // 2
    first, high, low = fourier_tables(pixels, orders, tile)
    rows0 = block * channels
    halves = []
    for s in range(steps):
        halves += [pltpu.VMEM((2, chunks, rows0 >> (s + 1), width), BF16)] * 2
    cfg = (maps, cycles, orders, ells, devices, grp, width)
    scratch = [
        pltpu.SMEM((orders,), jnp.int32),
        pltpu.VMEM((1, orders), jnp.int32),
        pltpu.VMEM((orders, tile), F32),
        pltpu.VMEM((chunks, cycles, orders, width), BF16),
        pltpu.VMEM((maps, cycles, coarse, tile), F32),
        pltpu.VMEM(first.shape, F32),
        pltpu.VMEM(high.shape, BF16),
        pltpu.VMEM(low.shape, BF16),
        pltpu.VMEM((orders, orders), BF16),
        pltpu.VMEM((2, 2, block // GROUP, GROUP * channels, 4 * cycles * GROUP), BF16),
        pltpu.VMEM((2, chunks, cycles, block, width), BF16),
        pltpu.VMEM((2, chunks, 3, cycles, block, width), BF16),
        pltpu.VMEM((2, chunks, 3, cycles, block, width), BF16),
        pltpu.VMEM((2, 2, GROUP, tile), BF16),
        pltpu.VMEM((2, 2, 3, GROUP, tile), BF16),
        pltpu.VMEM((2, 2, 3, GROUP, tile), BF16),
        pltpu.VMEM((2, chunks, rows0 // 2, width), F32),
        halves,
        pltpu.VMEM((tiles, pairs, tile), F32),
        pltpu.VMEM((tiles, pairs, tile), F32),
        pltpu.VMEM((pairs, tile), F32),
        pltpu.VMEM((sharers - 1, pairs, tile), F32),
        pltpu.VMEM((pairs, tile), F32),
        pltpu.VMEM((devices, pairs, tile), F32),
        pltpu.SemaphoreType.DMA((4,)),
        pltpu.SemaphoreType.DMA,
        pltpu.SemaphoreType.DMA((5,)),
        pltpu.SemaphoreType.DMA((4 + steps,)),
        pltpu.SemaphoreType.DMA((SLOTS, 2)),
        pltpu.SemaphoreType.DMA((2, 2)),
        pltpu.SemaphoreType.DMA((steps, SLOTS, 2)),
        pltpu.SemaphoreType.DMA((2,)),
        pltpu.SemaphoreType.DMA((2, sharers - 1)),
    ]
    anywhere = pl.BlockSpec(memory_space=pl.ANY)
    vmem = pl.BlockSpec(memory_space=pltpu.VMEM)
    harmonics, spectra = pl.pallas_call(
        functools.partial(kernel, cfg),
        out_shape=[
            pltpu.VMEM((own * maps, 2, ells), F32),
            pltpu.VMEM((pairs, ells // devices), F32),
        ],
        in_specs=[anywhere] * 7,
        out_specs=[vmem, vmem],
        scratch_shapes=scratch,
        compiler_params=pltpu.CompilerParams(
            vmem_limit_bytes=56 * MIB, collective_id=0, has_side_effects=True
        ),
        cost_estimate=pl.CostEstimate(
            flops=2 * cycles * orders * orders * ells, bytes_accessed=2 * legendre.size, transcendentals=0
        ),
    )(
        owner_table,
        owner_table.reshape(1, orders),
        sky_maps,
        jnp.asarray(first),
        jnp.asarray(high),
        jnp.asarray(low),
        legendre,
    )
    harmonics, spectra = (pltpu.with_memory_space_constraint(v, pltpu.VMEM) for v in (harmonics, spectra))
    harmonics, spectra = hand_over(harmonics, spectra)
    return harmonics.reshape(own, maps, 2, ells), spectra


def solution(mesh):
    return jax.shard_map(
        per_device,
        mesh=mesh,
        in_specs=(P(None, AXES, None), P(AXES, None, None), P()),
        out_specs=(P(AXES, None, None, None), P(None, AXES)),
        check_vma=False,
    )
```

```python
import functools
import math

import jax
import jax.numpy as jnp
import numpy as np
from jax import lax
from jax.experimental import pallas as pl
from jax.experimental.pallas import tpu as pltpu
from jax.sharding import PartitionSpec as P

AXES = ("blk", "grp")
MIB = 1024 * 1024
MESH = pl.DeviceIdType.MESH
BF16 = jnp.bfloat16
F32 = jnp.float32
GROUP = 16
FIRST = (1, 2)
EARLY = 3
WIDTH = 128
AHEAD = 3
CROSS = 1
SWAPPED = 1
FINALE = (
    *((1, 4), (0, 2), (3, 9), (3, 8), (1, 3), (0, 1), (2, 6), (2, 5), (3, 7), (2, 4), (2, 3)),
    *((1, 2), (1, 1), (3, 6), (2, 2), (3, 5), (2, 1), (3, 4), (3, 3), (3, 2), (3, 1)),
)
ROTATE = 0
SLOTS = 8
LAGS = (2, 2, 3)


def plan_of(bits):
    later = [[EARLY] + [b for b in range(1, bits) if b not in (first, EARLY)] for first in FIRST]
    return later


def flip(me, bits):
    out = me
    for b in bits:
        out = out + (1 - 2 * ((me // (1 << b)) % 2)) * (1 << b)
    return out


def split_bf16(values):
    high = values.astype(BF16)
    low = (values - high.astype(F32)).astype(BF16)
    return high, low


def dot(left, right):
    return jnp.dot(left, right, preferred_element_type=F32)


def dot_t(left, right):
    return lax.dot_general(left, right, (((1,), (1,)), ((), ())), preferred_element_type=F32)


def fourier_tables(pixels, order_count, width):
    coarse = pixels // width
    k1, m1 = np.meshgrid(np.arange(coarse), np.arange(coarse), indexing="ij")
    angle = 2.0 * math.pi * ((k1 * m1) % coarse) / coarse
    first = np.concatenate([np.cos(angle.T), -np.sin(angle.T)], axis=0)
    k2 = np.arange(width)[:, None]
    m = np.arange(order_count)[None, :]
    angle = 2.0 * math.pi * ((k2 * m) % pixels) / pixels
    cosine, sine = np.cos(angle) / math.sqrt(pixels), np.sin(angle) / math.sqrt(pixels)
    second = np.block([[cosine, -sine], [sine, cosine]]).astype(np.float32)
    high = second.astype(jnp.bfloat16)
    low = (second - high.astype(np.float32)).astype(jnp.bfloat16)
    return first.astype(np.float32), high, low


def kernel(
    cfg, owner_hbm, owner_row_hbm, sky_hbm, first_hbm, high_hbm, low_hbm, leg_hbm, harm_ref, spec_ref,
    owner_smem, owner_ref, column_v, leg_v, sky_v, first_v, high_v, low_v, hot_v, lhs_v, own0, send0, recv0, coef_own, coef_send, coef_recv,
    acc_v, halves, pow_v, pow_recv, pow_mine, pow_pair, pow_total, pow_direct, load_sem, sky_sem, table_sem,
    sent_sems, sems0, coef_sems, half_sems, pow_sems, pair_sems,
):
    maps, cycles, orders, ells, devices, grp, width = cfg
    bits = devices.bit_length() - 1
    later = plan_of(bits)
    steps = bits - 2
    chunks = ells // width
    channels = 2 * maps
    own = orders // devices
    per_type = own // 2
    block = orders // 8
    rows0 = block * channels
    me = lax.axis_index("blk") * grp + lax.axis_index("grp")
    tile = 128
    tiles = ells // tile
    sharers = tile * devices // ells
    pairs = maps * (maps + 1) // 2

    def at(index):
        return (index // grp, index % grp)

    def bit(b):
        return (me // (1 << b)) % 2

    gather = [
        [[None, flip(me, [0]), flip(me, [b]), flip(me, [b, 0])] for b in firsts] for firsts in (FIRST, (EARLY, EARLY))
    ]
    near = sorted({(b,) for b in range(bits)} | {(0, b) for b in FIRST + (EARLY,)}, reverse=True)

    def group_row(variant, p, g):
        q = p * 4 + g if variant == 0 else (g // 2) * 8 + (p % 2) * 4 + (p // 2) * 2 + g % 2
        return q * GROUP

    scope = jax.named_scope
    row_load = pltpu.make_async_copy(owner_row_hbm, owner_ref, table_sem.at[3])
    row_load.start()
    barrier = pltpu.get_barrier_semaphore()
    for masks in near:
        pl.semaphore_signal(barrier, inc=1, device_id=at(flip(me, masks)), device_id_type=MESH)

    def place_of(t):
        return (t + ROTATE * chunks // 16) % chunks

    def load(t):
        lanes = pl.ds(pl.multiple_of(place_of(t) * width, width), width)
        return pltpu.make_async_copy(leg_hbm.at[:, :, lanes], leg_v.at[t], load_sem.at[t % 4])

    def load_start(t, carry):
        load(t).start()
        return carry

    with scope("startload"):
        lax.fori_loop(0, 4, load_start, 0)
    coarse = sky_v.shape[2]

    def sky_load(k):
        lanes = pl.ds(k * tile, tile)
        return pltpu.make_async_copy(sky_hbm.at[:, :, lanes], sky_v.at[:, :, k, :], sky_sem)

    for k in range(coarse):
        sky_load(k).start()
    tables = [
        pltpu.make_async_copy(src, dst, table_sem.at[i])
        for i, (src, dst) in enumerate(((first_hbm, first_v), (high_hbm, high_v), (low_hbm, low_v)))
    ]
    for table in tables:
        table.start()


    half_bit, block_bit = (orders // 2).bit_length() - 1, block.bit_length() - 1

    def place(b, differs):
        mine = bit(b)
        return (mine + differs - 2 * mine * differs) * ((1 << b) * own)

    lane = lax.broadcasted_iota(jnp.int32, (orders, tile), 1)
    if per_type % 8 == 0:
        places = [[place(b, differs) for differs in range(2)] for b in range(bits)]
        row_load.wait()
        for c in range(orders // tile):
            row = owner_ref[:, c * tile : (c + 1) * tile].astype(F32)
            column_v[c * tile : (c + 1) * tile, :] = jnp.broadcast_to(row, (tile, tile)).T
        picked = []
        for jb in range(0, orders, 8):
            ty = jb >> half_bit
            start = ty * per_type + jb % per_type + places[0][(jb >> block_bit) & 1]
            start = start + places[FIRST[ty]][(jb >> (block_bit + 1)) & 1]
            for s, b in enumerate(later[ty]):
                start = start + places[b][(jb >> (block_bit - s - 1)) & 1]
            picked.append(column_v[pl.ds(pl.multiple_of(start, 8), 8), :])
        column = jnp.concatenate(picked, axis=0)
        lane = lane.astype(F32)
        for c in range(orders // tile):
            hot_v[:, c * tile : (c + 1) * tile] = jnp.where(column == lane + float(c * tile), 1.0, 0.0).astype(BF16)
    else:
        j = lax.broadcasted_iota(jnp.int32, (orders, tile), 0)
        part = j >> half_bit
        slot = part * per_type + (j & (per_type - 1)) + place(0, (j >> block_bit) & 1)
        for ty in range(2):
            terms = place(FIRST[ty], (j >> (block_bit + 1)) & 1)
            for s, b in enumerate(later[ty]):
                terms = terms + place(b, (j >> (block_bit - s - 1)) & 1)
            slot = slot + jnp.where(part == ty, terms, 0)
        pick = jnp.concatenate(
            [jnp.where(slot == lane + c * tile, 1.0, 0.0).astype(BF16) for c in range(orders // tile)], axis=1
        )
        row_load.wait()
        index = lax.broadcasted_iota(jnp.int32, (orders, orders), 0)
        table = jnp.where(index == owner_ref[...], 1.0, 0.0).astype(BF16)
        hot_v[...] = dot_t(pick, table).astype(BF16)

    def whole(ref, sem):
        return pltpu.make_async_copy(ref, ref, sem)

    def gather_copy(ty, t, p, variant):
        return pltpu.make_async_remote_copy(
            src_ref=send0.at[ty, t, p - 1],
            dst_ref=recv0.at[ty, t, p - 1],
            send_sem=sent_sems.at[0],
            recv_sem=sems0.at[t % SLOTS, ty],
            device_id=at(gather[variant][ty][p]),
            device_id_type=MESH,
        )

    def coef_copy(variant, ty, p):
        return pltpu.make_async_remote_copy(
            src_ref=coef_send.at[variant, ty, p - 1],
            dst_ref=coef_recv.at[variant, ty, p - 1],
            send_sem=sent_sems.at[1],
            recv_sem=coef_sems.at[variant, ty],
            device_id=at(gather[variant][ty][p]),
            device_id_type=MESH,
        )

    swap_from = chunks - SWAPPED
    groups = block // GROUP

    def half_copy(s, ty, t):
        partner = flip(me, [later[ty][s]])
        if s < 2:
            partner = jnp.where(t < swap_from, partner, flip(me, [later[ty][1 - s]]))
        if s == 0:
            partner = jnp.where(t == CROSS, flip(me, [FIRST[ty]]), partner)
        return pltpu.make_async_remote_copy(
            src_ref=halves[2 * s].at[ty, t],
            dst_ref=halves[2 * s + 1].at[ty, t],
            send_sem=sent_sems.at[2 + s],
            recv_sem=half_sems.at[s, t % SLOTS, ty],
            device_id=at(partner),
            device_id_type=MESH,
        )

    def enter():
        with jax.named_scope("barrier"):
            pl.semaphore_wait(barrier, len(near))

    def permute(t, variant=0, entered=False):
        with jax.named_scope("load"):
            load(t).wait()
        with jax.named_scope("permute"):
            permute_loaded(t, variant)
        if entered:
            enter()
        for p in (2, 3, 1):
            for ty in range(2):
                gather_copy(ty, t, p, variant).start()

        @pl.when(t + 4 < chunks)
        def _():
            load(t + 4).start()

    def permute_loaded(t, variant):
        together = max(1, 256 // width)
        for r0 in range(0, cycles, together):
            values = jnp.concatenate([leg_v[t, r0 + i] for i in range(together)], axis=1)
            for ty in range(2):
                picked = dot(hot_v[ty * 4 * block : (ty + 1) * 4 * block, :], values).astype(BF16)
                for i in range(together):
                    piece = picked[:, i * width : (i + 1) * width]
                    for p in range(4):
                        rows = [group_row(variant, p, g) for g in range(groups)]
                        rows = jnp.concatenate([piece[row : row + GROUP] for row in rows], axis=0)
                        if p == 0:
                            own0[ty, t, r0 + i] = rows
                        else:
                            send0[ty, t, p - 1, r0 + i] = rows

    permute(0, entered=True)
    permute(CROSS, 1)
    order_load = pltpu.make_async_copy(owner_hbm, owner_smem, table_sem.at[4])
    order_load.start()

    with jax.named_scope("waitsky"):
        whole(sky_v, sky_sem).wait()
    for table in tables:
        table.wait()
    count = maps * cycles
    columns = 2 * orders
    stages = []
    pixels = jnp.concatenate([sky_v[b // cycles, b % cycles] for b in range(count)], axis=1)
    stage = jnp.dot(first_v[...], pixels, precision=lax.Precision.HIGHEST, preferred_element_type=F32)
    for b in range(count):
        lanes = slice(b * tile, (b + 1) * tile)
        stages.append(jnp.concatenate([stage[:coarse, lanes], stage[coarse:, lanes]], axis=1))
    left_high, left_low = split_bf16(jnp.concatenate(stages, axis=0))
    spectral = []
    span = orders // 2
    for c in range(columns // span):
        picked = slice(c * span, (c + 1) * span)
        full = dot(left_high, high_v[:, picked]) + (dot(left_high, low_v[:, picked]) + dot(left_low, high_v[:, picked]))
        full = full.reshape(count, coarse, span)
        m1 = lax.broadcasted_iota(jnp.int32, (1, coarse, span), 1)
        col = lax.broadcasted_iota(jnp.int32, (1, coarse, span), 2)
        spectral.append(jnp.sum(jnp.where(col % coarse == m1, full, 0.0), axis=1))
    spectral = jnp.concatenate(
        [jnp.concatenate(spectral[:2], axis=1), jnp.concatenate(spectral[2:], axis=1)], axis=0
    ).astype(BF16)
    copies = tile // (2 * count)
    coef = dot_t(hot_v[...], jnp.concatenate([spectral] * copies, axis=0))
    lane_group = lax.broadcasted_iota(jnp.int32, (GROUP, tile), 1) // (2 * count)
    for variant in range(2):
        for ty in range(2):
            for p in range(4):
                packed = None
                for g in range(groups):
                    row = ty * 4 * block + group_row(variant, p, g)
                    rows = coef[row : row + GROUP]
                    packed = rows if packed is None else jnp.where(lane_group == g, rows, packed)
                if p == 0:
                    coef_own[variant, ty] = packed.astype(BF16)
                else:
                    coef_send[variant, ty, p - 1] = packed.astype(BF16)
    for variant in range(2):
        for p in (2, 3, 1):
            for ty in range(2):
                coef_copy(variant, ty, p).start()

    order_load.wait()

    def permute_step(t, carry):
        permute(t)
        return carry

    lax.fori_loop(CROSS + 1, AHEAD + 1, permute_step, 0)

    source = lax.broadcasted_iota(jnp.int32, (tile, cycles * tile), 0)
    target = lax.broadcasted_iota(jnp.int32, (tile, cycles * tile), 1)
    channel = 2 * ((source // cycles) % maps) + (source // count) % 2
    same = (source % cycles == target // tile) & (channel == target % channels)
    expand = jnp.where(same, 1.0, 0.0).astype(BF16)
    depth = 4 * cycles * GROUP
    keep = lax.broadcasted_iota(jnp.int32, (depth, tile), 0) % GROUP == (
        lax.broadcasted_iota(jnp.int32, (depth, tile), 1) // channels
    )
    pack_group = lax.broadcasted_iota(jnp.int32, (4 * GROUP, tile), 1) // (2 * count)

    def build(variant):
        for ty in range(2):
            with scope("waitcoef"):
                whole(coef_recv.at[variant, ty], coef_sems.at[variant, ty]).wait()
            values = [coef_own[variant, ty]] + [coef_recv[variant, ty, p] for p in range(3)]
            values = jnp.concatenate(values, axis=0).astype(F32)
            for g in range(groups):
                spread = dot(jnp.where(pack_group == g, values, 0.0).astype(BF16), expand)
                pieces = [
                    spread[p * GROUP : (p + 1) * GROUP, r * tile : (r + 1) * tile]
                    for p in range(4)
                    for r in range(cycles)
                ]
                stacked = jnp.where(keep, jnp.concatenate(pieces, axis=0), 0.0)
                lhs_v[variant, ty, g] = stacked.T.astype(BF16)

    build(0)
    high_rows = GROUP * channels

    def product(variant, ty, t, g):
        span = slice(g * GROUP, (g + 1) * GROUP)
        parts = [own0[ty, t, :, span, :]] + [recv0[ty, t, p, :, span, :] for p in range(3)]
        right = jnp.concatenate([v.reshape(cycles * GROUP, width) for v in parts], axis=0)
        return dot(lhs_v[variant, ty, g], right)

    def first_step(t, sent, kept, variant=0):
        for ty in range(2):
            with jax.named_scope("wait0"):
                whole(recv0.at[ty, t], sems0.at[t % SLOTS, ty]).wait()
            for i, g in enumerate(sent):
                halves[0][ty, t, i * high_rows : (i + 1) * high_rows, :] = product(variant, ty, t, g).astype(BF16)
            half_copy(0, ty, t).start()
        for ty in range(2):
            for i, g in enumerate(kept):
                acc_v[ty, t, i * high_rows : (i + 1) * high_rows, :] = product(variant, ty, t, g)

    def next_step(s, t):
        size = rows0 >> (s + 1)
        for ty in range(2):
            with jax.named_scope(f"wait{s}"):
                half_copy(s - 1, ty, t).wait_recv()
            got = halves[2 * s - 1]
            value = acc_v[ty, t, size : 2 * size, :] + got[ty, t, size:, :].astype(F32)
            halves[2 * s][ty, t] = value.astype(BF16)
            half_copy(s, ty, t).start()
            acc_v[ty, t, :size, :] = acc_v[ty, t, :size, :] + got[ty, t, :size, :].astype(F32)

    def pow_copy(u):
        return pltpu.make_async_remote_copy(
            src_ref=pow_v.at[u],
            dst_ref=pow_recv.at[me // sharers],
            send_sem=sent_sems.at[2 + steps],
            recv_sem=pow_sems.at[0],
            device_id=at(u * sharers + me % sharers),
            device_id_type=MESH,
        )

    def direct_copy(u, owner):
        return pltpu.make_async_remote_copy(
            src_ref=pow_v.at[u],
            dst_ref=pow_direct.at[me],
            send_sem=sent_sems.at[3 + steps],
            recv_sem=pow_sems.at[1],
            device_id=at(owner),
            device_id_type=MESH,
        )

    def last_step(t, direct=False):
        size = rows0 >> steps
        ell = place_of(t) * width + lax.broadcasted_iota(jnp.int32, (channels, width), 1)
        total = [None] * (maps // 2 + 1)
        lanes = pl.ds(pl.multiple_of(place_of(t) * width, width), width)
        for ty in range(2):
            with jax.named_scope("waitlast"):
                half_copy(steps - 1, ty, t).wait_recv()
            value = acc_v[ty, t, :size, :] + halves[2 * steps - 1][ty, t].astype(F32)
            for i in range(per_type):
                order = owner_smem[me * own + ty * per_type + i]
                mode = jnp.where(ell >= order, value[i * channels : (i + 1) * channels], 0.0)
                row = (ty * per_type + i) * maps
                for a in range(maps):
                    harm_ref[row + a, :, lanes] = mode[2 * a : 2 * a + 2]
                heavy = mode * jnp.where(order == 0, 1.0, 2.0)
                for k in range(maps // 2 + 1):
                    turned = mode if k == 0 else jnp.concatenate([mode[2 * k :], mode[: 2 * k]], axis=0)
                    term = heavy * turned
                    total[k] = term if total[k] is None else total[k] + term
        rows = []
        for i in range(maps):
            for jj in range(i, maps):
                k, a = (jj - i, i) if jj - i <= maps // 2 else (maps - (jj - i), jj)
                rows.append(total[k][2 * a : 2 * a + 1] + total[k][2 * a + 1 : 2 * a + 2])
        power = jnp.concatenate(rows, axis=0)
        for h in range(width // tile):
            u = place_of(t) * (width // tile) + h
            pow_v[u] = power[:, h * tile : (h + 1) * tile]

            if direct:
                for e in range(sharers):

                    @pl.when(u * sharers + e != me)
                    def _():
                        direct_copy(u, u * sharers + e).start()

            else:

                @pl.when(u != me // sharers)
                def _():
                    pow_copy(u).start()

    lags = [0, LAGS[0]]
    for s in range(2, steps):
        lags.append(lags[-1] + LAGS[1])
    end = lags[-1] + LAGS[2]

    def first_of(t):
        @pl.when((t < swap_from) & (t != CROSS))
        def _():
            with scope("first"):
                first_step(t, (2, 3), (0, 1))

        @pl.when(t == CROSS)
        def _():
            with scope("build"):
                build(1)
            with scope("first"):
                first_step(t, (2, 3), (0, 1), 1)

        @pl.when((t >= swap_from) & (t < chunks))
        def _():
            with scope("first"):
                first_step(t, (1, 3), (0, 2))

    def later_of(t):
        for s in range(1, steps):

            @pl.when((t >= lags[s]) & (t < chunks + lags[s]))
            def _():
                with scope(f"next{s}"):
                    next_step(s, t - lags[s])

        @pl.when(t >= end)
        def _():
            with scope("last"):
                last_step(t - end)

    def main(t, carry):
        @pl.when((t > 0) & (t + AHEAD < chunks))
        def _():
            permute(t + AHEAD)

        first_of(t)
        later_of(t)
        return carry

    special = steps == 3 and chunks >= 14
    lax.fori_loop(0, chunks - 2 if special else chunks + end, main, 0)
    if special:
        with scope("finale"):
            for e, back in FINALE:
                t = chunks - back
                with scope(f"e{e}"):
                    if e == 0:
                        first_step(t, (1, 3) if back <= SWAPPED else (2, 3), (0, 2) if back <= SWAPPED else (0, 1))
                    elif e < 3:
                        next_step(e, t)
                    else:
                        last_step(t, direct=back == 1)

    mine = me // sharers
    straight = (tiles - 1 + ROTATE) % tiles if special else tiles

    def pair_copy(e):
        return pltpu.make_async_remote_copy(
            src_ref=pow_mine,
            dst_ref=pow_pair.at[e - 1],
            send_sem=pair_sems.at[0, e - 1],
            recv_sem=pair_sems.at[1, e - 1],
            device_id=at(mine * sharers + (me + e) % sharers),
            device_id_type=MESH,
        )

    @pl.when(mine != straight)
    def _():
        with scope("waitpow"):
            whole(pow_recv.at[: tiles - 1], pow_sems.at[0]).wait()
        total = pow_v[mine]
        for u in range(tiles):
            total = total + jnp.where(u != mine, pow_recv[u], 0.0)
        pow_mine[...] = total
        for e in range(1, sharers):
            pair_copy(e).start()
        with scope("waitpair"):
            for e in range(1, sharers):
                pair_copy(e).wait_recv()
                total = total + pow_pair[e - 1]
        pow_total[...] = total

    if special:

        @pl.when(mine == straight)
        def _():
            with scope("waitpow"):
                whole(pow_direct.at[: devices - 1], pow_sems.at[1]).wait()
            total = pow_v[mine]
            for d in range(devices):
                total = total + jnp.where(d != me, pow_direct[d], 0.0)
            pow_total[...] = total

    total = pow_total[...]
    ell = mine * tile + lax.broadcasted_iota(jnp.int32, total.shape, 1)
    total = total / (2 * ell + 1).astype(F32)
    share = tile // sharers
    turned = total
    for c in range(1, sharers):
        shifted = jnp.concatenate([total[:, c * share :], total[:, : c * share]], axis=1)
        turned = jnp.where(me % sharers == c, shifted, turned)
    spec_ref[...] = turned[:, :share]

    with jax.named_scope("drain"):
        whole(send0, sent_sems.at[0]).wait()
        whole(coef_send, sent_sems.at[1]).wait()
        for s in range(steps):
            whole(halves[2 * s], sent_sems.at[2 + s]).wait()
    if special:

        @pl.when(mine == straight)
        def _():
            whole(pow_v.at[: tiles - 1], sent_sems.at[2 + steps]).wait()
            whole(pow_v.at[: sharers - 1], sent_sems.at[3 + steps]).wait()

        @pl.when(mine != straight)
        def _():
            whole(pow_v.at[: tiles - 2], sent_sems.at[2 + steps]).wait()
            whole(pow_v.at[:sharers], sent_sems.at[3 + steps]).wait()

    else:
        whole(pow_v.at[: tiles - 1], sent_sems.at[2 + steps]).wait()

    @pl.when(mine != straight)
    def _():
        for e in range(1, sharers):
            pair_copy(e).wait_send()


def hand_over_body(large_ref, small_ref, large_out, small_out, sems):
    copies = [
        pltpu.make_async_copy(large_ref, large_out, sems.at[0]),
        pltpu.make_async_copy(small_ref, small_out, sems.at[1]),
    ]
    for copy in copies:
        copy.start()
    for copy in copies:
        copy.wait()


def hand_over(large, small):
    return pl.pallas_call(
        hand_over_body,
        out_shape=[jax.ShapeDtypeStruct(large.shape, large.dtype), jax.ShapeDtypeStruct(small.shape, small.dtype)],
        in_specs=[pl.BlockSpec(memory_space=pltpu.VMEM)] * 2,
        out_specs=[pl.BlockSpec(memory_space=pl.ANY)] * 2,
        scratch_shapes=[pltpu.SemaphoreType.DMA((2,))],
        cost_estimate=pl.CostEstimate(flops=large.size, bytes_accessed=8 * large.size, transcendentals=0),
    )(large, small)


def per_device(sky_maps, legendre, owner_table):
    maps, cycles, pixels = sky_maps.shape
    _, orders, ells = legendre.shape
    devices = lax.axis_size(AXES)
    grp = lax.axis_size(AXES[1])
    bits = devices.bit_length() - 1
    steps = bits - 2
    width = WIDTH
    chunks = ells // width
    channels = 2 * maps
    own = orders // devices
    block = orders // 8
    tile = 128
    coarse = pixels // tile
    tiles = ells // tile
    sharers = tile * devices // ells
    pairs = maps * (maps + 1) // 2
    first, high, low = fourier_tables(pixels, orders, tile)
    rows0 = block * channels
    halves = []
    for s in range(steps):
        halves += [pltpu.VMEM((2, chunks, rows0 >> (s + 1), width), BF16)] * 2
    cfg = (maps, cycles, orders, ells, devices, grp, width)
    scratch = [
        pltpu.SMEM((orders,), jnp.int32),
        pltpu.VMEM((1, orders), jnp.int32),
        pltpu.VMEM((orders, tile), F32),
        pltpu.VMEM((chunks, cycles, orders, width), BF16),
        pltpu.VMEM((maps, cycles, coarse, tile), F32),
        pltpu.VMEM(first.shape, F32),
        pltpu.VMEM(high.shape, BF16),
        pltpu.VMEM(low.shape, BF16),
        pltpu.VMEM((orders, orders), BF16),
        pltpu.VMEM((2, 2, block // GROUP, GROUP * channels, 4 * cycles * GROUP), BF16),
        pltpu.VMEM((2, chunks, cycles, block, width), BF16),
        pltpu.VMEM((2, chunks, 3, cycles, block, width), BF16),
        pltpu.VMEM((2, chunks, 3, cycles, block, width), BF16),
        pltpu.VMEM((2, 2, GROUP, tile), BF16),
        pltpu.VMEM((2, 2, 3, GROUP, tile), BF16),
        pltpu.VMEM((2, 2, 3, GROUP, tile), BF16),
        pltpu.VMEM((2, chunks, rows0 // 2, width), F32),
        halves,
        pltpu.VMEM((tiles, pairs, tile), F32),
        pltpu.VMEM((tiles, pairs, tile), F32),
        pltpu.VMEM((pairs, tile), F32),
        pltpu.VMEM((sharers - 1, pairs, tile), F32),
        pltpu.VMEM((pairs, tile), F32),
        pltpu.VMEM((devices, pairs, tile), F32),
        pltpu.SemaphoreType.DMA((4,)),
        pltpu.SemaphoreType.DMA,
        pltpu.SemaphoreType.DMA((5,)),
        pltpu.SemaphoreType.DMA((4 + steps,)),
        pltpu.SemaphoreType.DMA((SLOTS, 2)),
        pltpu.SemaphoreType.DMA((2, 2)),
        pltpu.SemaphoreType.DMA((steps, SLOTS, 2)),
        pltpu.SemaphoreType.DMA((2,)),
        pltpu.SemaphoreType.DMA((2, sharers - 1)),
    ]
    anywhere = pl.BlockSpec(memory_space=pl.ANY)
    vmem = pl.BlockSpec(memory_space=pltpu.VMEM)
    harmonics, spectra = pl.pallas_call(
        functools.partial(kernel, cfg),
        out_shape=[
            pltpu.VMEM((own * maps, 2, ells), F32),
            pltpu.VMEM((pairs, ells // devices), F32),
        ],
        in_specs=[anywhere] * 7,
        out_specs=[vmem, vmem],
        scratch_shapes=scratch,
        compiler_params=pltpu.CompilerParams(
            vmem_limit_bytes=56 * MIB, collective_id=0, has_side_effects=True
        ),
        cost_estimate=pl.CostEstimate(
            flops=2 * cycles * orders * orders * ells, bytes_accessed=2 * legendre.size, transcendentals=0
        ),
    )(
        owner_table,
        owner_table.reshape(1, orders),
        sky_maps,
        jnp.asarray(first),
        jnp.asarray(high),
        jnp.asarray(low),
        legendre,
    )
    harmonics, spectra = (pltpu.with_memory_space_constraint(v, pltpu.VMEM) for v in (harmonics, spectra))
    harmonics, spectra = hand_over(harmonics, spectra)
    return harmonics.reshape(own, maps, 2, ells), spectra


def solution(mesh):
    return jax.shard_map(
        per_device,
        mesh=mesh,
        in_specs=(P(None, AXES, None), P(AXES, None, None), P()),
        out_specs=(P(AXES, None, None, None), P(None, AXES)),
        check_vma=False,
    )
```
